16 devices in a mesh: dp: 1, ep: 16 (over x, y, z, core).
Axes of the slice: x: 2, y: 2, z: 2, core: 2. Of those that a mesh axis runs over, the one named last changes fastest.
Arguments:
- x: bfloat16 [1, 16, 256, 2048], P('dp', 'ep')
- expert: int32 [1, 16, 256, 6], P('dp', 'ep')
- slot: int32 [1, 16, 256, 6], P('dp', 'ep')
- gate: float32 [1, 16, 256, 6], P('dp', 'ep')
- w_gate: bfloat16 [64, 2048, 1408], P('ep')
- w_up: bfloat16 [64, 2048, 1408], P('ep')
- w_down: bfloat16 [64, 1408, 2048], P('ep')
- s_gate: bfloat16 [2048, 2816], replicated
- s_up: bfloat16 [2048, 2816], replicated
- s_down: bfloat16 [2816, 2048], replicated
Outputs:
- y: bfloat16 [1, 16, 256, 2048], P('dp', 'ep')
All inputs are finite; a program needn't handle non-finite values.
Results may differ from the reference program's by a relative error of at most 0.009.
Values are sent between devices in bfloat16 or wider.
A program may use at most 2 GiB of HBM per device.

```python
import jax
import jax.numpy as jnp

MEMBERS = 16
TOKENS = 256
D = 2048
FF = 1408
TOP = 6
EXPERTS = 64
SHARED_FF = 2816
SLOTS = 5 * TOKENS * TOP // (4 * EXPERTS)


def setup_inputs(seed: int = 0, part: int = 0) -> dict:
    own, k1, k2, k3, k4, k5, k6 = jax.random.split(jax.random.key(seed), 7)
    kx, ke, kl, kg = jax.random.split(jax.random.fold_in(own, part), 4)
    devices = (1, MEMBERS)
    place = jax.random.permutation(kl, jnp.arange(EXPERTS, dtype=jnp.uint32))
    slow = ((EXPERTS + (9 * place) % EXPERTS) << ((9 * place) // EXPERTS)) // EXPERTS
    wait = (jax.random.bits(ke, (*devices, TOKENS, EXPERTS), jnp.uint32) >> 10) * slow
    expert = jnp.argsort(wait, axis=-1)[..., :TOP].astype(jnp.int32)
    chosen = jax.nn.one_hot(expert, EXPERTS, dtype=jnp.int32)
    in_line = jnp.cumsum(chosen.reshape(*devices, TOKENS * TOP, EXPERTS), axis=2) - 1
    slot = jnp.sum(in_line.reshape(chosen.shape) * chosen, axis=-1)

    def one(key, rows, columns):
        return (jax.random.normal(key, (rows, columns), jnp.float32) * rows**-0.5).astype(jnp.bfloat16)

    def weights(key, rows, columns):
        return jax.lax.map(lambda k: one(k, rows, columns), jax.random.split(key, EXPERTS))

    return {
        "x": jax.random.normal(kx, (*devices, TOKENS, D), jnp.float32).astype(jnp.bfloat16),
        "expert": expert,
        "slot": slot,
        "gate": jax.nn.softmax(jax.random.normal(kg, expert.shape, jnp.float32)),
        "w_gate": weights(k1, D, FF),
        "w_up": weights(k2, D, FF),
        "w_down": weights(k3, FF, D),
        "s_gate": one(k4, D, SHARED_FF),
        "s_up": one(k5, D, SHARED_FF),
        "s_down": one(k6, SHARED_FF, D),
    }


def einsum(form, a, b):
    return jnp.einsum(form, a.astype(jnp.float32), b.astype(jnp.float32))


def for_all(x, s_gate, s_up, s_down):
    h = jax.nn.silu(einsum("...d,df->...f", x, s_gate)) * einsum("...d,df->...f", x, s_up)
    return einsum("...f,fd->...d", h.astype(jnp.bfloat16), s_down)


def reference(x, expert, slot, gate, w_gate, w_up, w_down, s_gate, s_up, s_down):
    to_expert = jax.nn.one_hot(expert, EXPERTS, dtype=jnp.bfloat16)
    to_slot = jax.nn.one_hot(slot, SLOTS, dtype=jnp.bfloat16)
    weighted = to_expert * gate[..., None].astype(jnp.bfloat16)
    dispatch = einsum("abtke,abtkc->abtec", to_expert, to_slot).astype(jnp.bfloat16)
    combine = einsum("abtke,abtkc->abtec", weighted, to_slot).astype(jnp.bfloat16)
    z = einsum("abtec,abtd->aebcd", dispatch, x).astype(jnp.bfloat16)
    h = jax.nn.silu(einsum("aebcd,edf->aebcf", z, w_gate))
    h = (h * einsum("aebcd,edf->aebcf", z, w_up)).astype(jnp.bfloat16)
    out = einsum("aebcf,efd->aebcd", h, w_down).astype(jnp.bfloat16)
    y = einsum("abtec,aebcd->abtd", combine, out)
    return (y + for_all(x, s_gate, s_up, s_down)).astype(jnp.bfloat16)
```

```python
import functools

import jax
import jax.numpy as jnp
from jax import lax
from jax.experimental import pallas as pl
from jax.experimental.pallas import tpu as pltpu
from jax.sharding import PartitionSpec as P

MESH = pl.DeviceIdType.MESH
F32, BF16 = jnp.float32, jnp.bfloat16

T, D, F, TOP = 256, 2048, 1408, 6
SLOTS, PAD, EXP = 30, 32, 4
ROWS = EXP * PAD
HALF = D // 2
PART = ((0, 88), (88, 88), (176, 80))
BIT = (4, 2, 1)
ORDER = tuple(tuple((p + i) % 3 for i in range(3)) for p in range(3))


def gather_messages(p):
    b0, b1, b2 = (BIT[d] for d in ORDER[p])
    table = ((0, 0), (0, 1), (b0, 1), (0, 2), (b0, 2), (b1, 2), (b0 | b1, 2))
    return tuple((s, i, s ^ BIT[ORDER[p][i]]) for s, i in table)


def scatter_messages(p):
    b0, b1, b2 = (BIT[d] for d in ORDER[p])
    return (
        (b0 | b1 | b2, 0, ()), (b0 | b1, 0, ()), (b0 | b2, 0, ()), (b0, 0, ()),
        (b1 | b2, 1, (0,)), (b1, 1, (1,)), (b2, 2, (2, 4)),
    )


GATHER = tuple(gather_messages(p) for p in range(3))
SCATTER = tuple(scatter_messages(p) for p in range(3))
N_TILES = tuple((n, min(256, F - n)) for n in range(0, F, 256))


def kernel(x, meta, wg, wu, wd, sg, su, sd, y, xg, *scratch):
    (gbuf, ubuf, dbuf, z, ob, dr, r0, r1, r2, s0, s1, s2, acc, xt, comb, h, fs, fr, mt,
     wsem, xsem, lsem, xs_s, xs_r, meta_s, meta_r, ag_s, ag_r, fw_s, fw_r, dr_s, dr_r, rs_s, rs_r, fin_s, fin_r) = scratch
    me = lax.axis_index("ep")
    c, q = me % 2, me // 2
    sib = me + 1 - 2 * c
    nbr = [me + (1 - 2 * ((me // (2 * b)) % 2)) * (2 * b) for b in BIT]
    mine = pl.ds(pl.multiple_of(c * HALF, HALF), HALF)
    theirs = pl.ds(pl.multiple_of((1 - c) * HALF, HALF), HALF)
    rbuf, sbuf = (r0, r1, r2), (s0, s1, s2)

    def remote(src, dst, send, recv, to):
        return pltpu.make_async_remote_copy(
            src_ref=src, dst_ref=dst, send_sem=send, recv_sem=recv, device_id={"ep": to}, device_id_type=MESH)

    def ag(k, p, m):
        s, i, land = GATHER[p][m]
        rows = pl.ds(*PART[p])
        return remote(xg.at[k, s, rows, mine], xg.at[k, land, rows, mine], ag_s.at[k, p, m], ag_r.at[k, p, m],
                      nbr[ORDER[p][i]])

    def fwd(k, p, m):
        rows = pl.ds(*PART[p])
        piece = xg.at[k, GATHER[p][m][2], rows, mine]
        return remote(piece, piece, fw_s.at[k, p, m], fw_r.at[k, p, m], sib)

    def fwd_in(k, p, m):
        rows = pl.ds(*PART[p])
        piece = xg.at[k, GATHER[p][m][2], rows, theirs]
        return remote(piece, piece, fw_s.at[k, p, m], fw_r.at[k, p, m], sib)

    def give(k, r):
        return remote(z.at[r // 2, :, pl.ds((r % 2) * HALF, HALF)], dr.at[k, r], dr_s.at[k, r], dr_r.at[k, r], sib)

    def rs(k, p, n):
        return remote(sbuf[p].at[n], rbuf[p].at[k, n], rs_s.at[k, p, n], rs_r.at[k, p, n],
                      nbr[ORDER[p][SCATTER[p][n][1]]])

    def meta_copy(i):
        return remote(meta, mt.at[i], meta_s.at[i], meta_r.at[i], xor(me, i, 4))

    def xor(v, mask, bits):
        out = v
        for b in range(bits):
            if mask >> b & 1:
                out = out + (1 - 2 * ((v // (1 << b)) % 2)) * (1 << b)
        return out

    own_send = remote(x, xg.at[c, 0], xs_s, xs_r, sib)
    own_recv = remote(x, xg.at[1 - c, 0], xs_s, xs_r, sib)
    x_in = pltpu.make_async_copy(x, xt.at[0], xsem.at[0])
    x_out = pltpu.make_async_copy(xt.at[0], xg.at[c, 0], lsem)
    final_send = remote(fs, fr, fin_s, fin_r, sib)

    def load_g(src):
        return pltpu.make_async_copy(src, gbuf, wsem.at[0])

    def load_u(src):
        return pltpu.make_async_copy(src, ubuf, wsem.at[1])

    def load_d(src):
        return pltpu.make_async_copy(src, dbuf, wsem.at[2])

    def shared_cols(ref, i):
        return ref.at[:, pl.ds(pl.multiple_of(i * F, 128), F)]

    def shared_rows(i):
        return sd.at[pl.ds(pl.multiple_of(i * F, 128), F), :]

    def start_gather(k):
        @pl.when(c != k)
        def _():
            own_recv.wait_recv()

        for m in (0, 1, 3):
            for p in range(3):
                ag(k, p, m).start()

    def arrive(k, m, sends):
        for p in range(3):
            ag(k, p, m).wait_recv()
            for n in sends:
                ag(k, p, n).start()
            fwd(k, p, m).start()

    def x_load(k, r, b):
        return pltpu.make_async_copy(xg.at[k, r], xt.at[b], xsem.at[b])

    def landed(k, r):
        for p in range(3):
            for m in range(7):
                if GATHER[p][m][2] == r:
                    fwd_in(k, p, m).wait_recv()

    def dispatch(k, r, b):
        x_load(k, r, b).wait()
        table = mt[2 * r + (k + c) % 2]
        row = (lax.broadcasted_iota(jnp.int32, (ROWS, T), 0) + me * ROWS).astype(F32)
        pick = jnp.zeros((ROWS, T), F32)
        weight = jnp.zeros((ROWS, T), F32)
        for j in range(TOP):
            hit = table[j:j + 1, :] == row
            pick = jnp.where(hit, 1.0, pick)
            weight = jnp.where(hit, table[8 + j:9 + j, :], weight)
        comb[k, r] = weight.T
        for n in range(0, D, 512):
            rows = jnp.dot(pick.astype(BF16), xt[b, :, n:n + 512], preferred_element_type=F32).astype(BF16)
            for e in range(EXP):
                z[e, r * PAD:(r + 1) * PAD, n:n + 512] = rows[e * PAD:(e + 1) * PAD]

    def hidden(load):
        for n, w in N_TILES:
            g = jnp.dot(load(), gbuf[:, n:n + w], preferred_element_type=F32)
            u = jnp.dot(load(), ubuf[:, n:n + w], preferred_element_type=F32)
            h[:, n:n + w] = (g * (1.0 / (1.0 + jnp.exp(-g))) * u).astype(BF16)

    def down(store):
        for n in range(0, D, 512):
            store(n, jnp.dot(h[...], dbuf[:, n:n + 512], preferred_element_type=F32))

    def give_all(k):
        for r in (7, 6, 5, 3, 4, 2, 1, 0):
            part = jnp.dot(comb[k, r].astype(BF16), ob[k, r, :, theirs], preferred_element_type=F32)
            z[r // 2, :, (r % 2) * HALF:(r % 2) * HALF + HALF] = part.astype(BF16)
            give(k, r).start()

    def term(k, p, r):
        first, rows = PART[p]
        low = first // 16 * 16
        part = jnp.dot(comb[k, r, first:first + rows, :].astype(BF16), ob[k, r, :, mine], preferred_element_type=F32)
        other = dr[k, r, low:first + rows, :].astype(F32)[first - low:]
        return part + other

    def send_sum(k, n):
        for p in range(3):
            r, _, joins = SCATTER[p][n]
            total = term(k, p, r)
            for j in joins:
                rs(k, p, j).wait_recv()
                total = total + rbuf[p][k, j].astype(F32)
            if k == 1:
                rs(0, p, n).wait_send()
            sbuf[p][n] = total.astype(BF16)
            rs(k, p, n).start()

    def start_scatter(k):
        give(k, 7).wait_recv()
        send_sum(k, 0)
        for r in (6, 5, 3):
            give(k, r).wait_recv()
        send_sum(k, 1)
        send_sum(k, 2)
        for r in (4, 2, 1):
            give(k, r).wait_recv()
        send_sum(k, 3)
        give(k, 0).wait_recv()

    def finish(k):
        for p in range(3):
            first, rows = PART[p]
            total = term(k, p, 0)
            for j in (3, 5, 6):
                rs(k, p, j).wait_recv()
                total = total + rbuf[p][k, j].astype(F32)

            @pl.when(c == k)
            def _():
                acc[first:first + rows, mine] += total

            @pl.when(c != k)
            def _():
                fs[p, :rows] = total.astype(BF16)

        @pl.when(c != k)
        def _():
            final_send.start()

    x_in.start()
    own_send.start()
    mt[0] = meta[...]
    load_g(shared_cols(sg, 0)).start()
    load_u(shared_cols(su, 0)).start()
    load_d(shared_rows(0)).start()
    for i in range(1, 16):
        meta_copy(i).start()
    x_in.wait()
    x_out.start()
    x_out.wait()
    start_gather(0)
    acc[...] = jnp.zeros_like(acc)

    @pl.loop(0, 2)
    def _(i):
        load_g(shared_cols(sg, i)).wait()
        load_u(shared_cols(su, i)).wait()
        hidden(lambda: xt[0])

        @pl.when(i == 0)
        def _():
            load_g(shared_cols(sg, 1)).start()
            load_u(shared_cols(su, 1)).start()

        @pl.when(i == 1)
        def _():
            load_g(wg.at[0]).start()
            load_u(wu.at[0]).start()
            arrive(0, 0, (2, 4))

        load_d(shared_rows(i)).wait()

        def store(n, v):
            acc[:, n:n + 512] += v

        down(store)

        @pl.when(i == 0)
        def _():
            load_d(shared_rows(1)).start()

        @pl.when(i == 1)
        def _():
            load_d(wd.at[0]).start()

    for i in range(1, 16):
        meta_copy(i).wait_recv()
    arrive(0, 1, (5,))
    x_load(0, 0, 0).start()
    arrive(0, 2, (6,))
    start_gather(1)
    arrive(0, 3, ())

    def dispatch_all(k, waits):
        order = (0, 4, 2, 1, 6, 5, 3, 7)
        for n, r in enumerate(order):
            if n + 1 < 8:
                nxt = order[n + 1]
                for m in waits.get(n + 1, ()):
                    arrive(k, m, ())
                landed(k, nxt)
                x_load(k, nxt, (n + 1) % 2).start()
            dispatch(k, r, n % 2)

    dispatch_all(0, {4: (4, 5), 7: (6,)})

    @pl.loop(0, 8)
    def _(i):
        k, e = i // 4, i % 4
        nxt = (i + 1) % 4
        load_g(wg.at[e]).wait()
        load_u(wu.at[e]).wait()
        hidden(lambda: z[e])

        @pl.when(i < 7)
        def _():
            load_g(wg.at[nxt]).start()
            load_u(wu.at[nxt]).start()

        @pl.when(i == 7)
        def _():
            send_sum(0, 6)

        load_d(wd.at[e]).wait()

        def store(n, v):
            for r in range(8):
                ob[k, r, pl.ds(pl.multiple_of(e * PAD, PAD), PAD), n:n + 512] = v[r * PAD:(r + 1) * PAD].astype(BF16)

        down(store)

        @pl.when(i < 7)
        def _():
            load_d(wd.at[nxt]).start()

        @pl.when(i == 0)
        def _():
            arrive(1, 0, (2, 4))

        @pl.when(i == 1)
        def _():
            arrive(1, 1, (5,))

        @pl.when(i == 2)
        def _():
            arrive(1, 2, (6,))
            arrive(1, 3, ())

        @pl.when(i == 3)
        def _():
            give_all(0)
            x_load(1, 0, 0).start()
            start_scatter(0)
            for r in range(8):
                give(0, r).wait_send()
            dispatch_all(1, {4: (4, 5), 7: (6,)})

        @pl.when(i == 4)
        def _():
            send_sum(0, 4)

        @pl.when(i == 5)
        def _():
            send_sum(0, 5)

    give_all(1)
    start_scatter(1)
    finish(0)
    send_sum(1, 4)
    send_sum(1, 5)
    send_sum(1, 6)
    finish(1)
    final_send.wait()
    for p in range(3):
        first, rows = PART[p]
        acc[first:first + rows, theirs] += fr[p, :rows].astype(F32)
    y[...] = acc[...].astype(BF16)

    own_send.wait_send()
    for i in range(1, 16):
        meta_copy(i).wait_send()
    for k in range(2):
        for p in range(3):
            for m in range(7):
                ag(k, p, m).wait_send()
                fwd(k, p, m).wait_send()
    for r in range(8):
        give(1, r).wait_send()
    for p in range(3):
        for n in range(7):
            rs(1, p, n).wait_send()


def solution(mesh):
    dma = pltpu.SemaphoreType.DMA

    def body(x, expert, slot, gate, wg, wu, wd, sg, su, sd):
        x = x.reshape(T, D)
        row = jnp.where(slot < SLOTS, expert * PAD + slot, -1).reshape(T, TOP).astype(F32)
        weight = gate.reshape(T, TOP).astype(BF16).astype(F32)
        blank = jnp.zeros((T, 8 - TOP), F32)
        meta = jnp.concatenate([row, blank, weight, blank], axis=1).T
        hbm, vmem = pl.BlockSpec(memory_space=pltpu.HBM), pl.BlockSpec(memory_space=pltpu.VMEM)
        y, _ = pl.pallas_call(
            kernel,
            name="moe",
            out_shape=(jax.ShapeDtypeStruct((T, D), BF16), jax.ShapeDtypeStruct((2, 8, T, D), BF16)),
            in_specs=[hbm, vmem, hbm, hbm, hbm, hbm, hbm, hbm],
            out_specs=(vmem, hbm),
            scratch_shapes=[
                pltpu.VMEM((D, F), BF16), pltpu.VMEM((D, F), BF16), pltpu.VMEM((F, D), BF16),
                pltpu.VMEM((EXP, T, D), BF16),
                pltpu.VMEM((2, 8, ROWS, D), BF16),
                pltpu.VMEM((2, 8, T, HALF), BF16),
                *[pltpu.VMEM((2, 7, n, HALF), BF16) for _, n in PART],
                *[pltpu.VMEM((7, n, HALF), BF16) for _, n in PART],
                pltpu.VMEM((T, D), F32),
                pltpu.VMEM((2, T, D), BF16),
                pltpu.VMEM((2, 8, T, ROWS), F32),
                pltpu.VMEM((T, F), BF16),
                pltpu.VMEM((3, 88, HALF), BF16), pltpu.VMEM((3, 88, HALF), BF16),
                pltpu.VMEM((16, 16, T), F32),
                dma((3,)), dma((2,)), dma, dma, dma, dma((16,)), dma((16,)),
                dma((2, 3, 7)), dma((2, 3, 7)), dma((2, 3, 7)), dma((2, 3, 7)),
                dma((2, 8)), dma((2, 8)), dma((2, 3, 7)), dma((2, 3, 7)), dma, dma,
            ],
            compiler_params=pltpu.CompilerParams(has_side_effects=True, vmem_limit_bytes=67_043_328),
        )(x, meta, wg, wu, wd, sg, su, sd)
        return y.reshape(1, 1, T, D)

    tokens, experts, whole = P("dp", "ep", None, None), P("ep", None, None), P(None, None)
    return jax.shard_map(
        body, mesh=mesh,
        in_specs=(tokens, tokens, tokens, tokens, experts, experts, experts, whole, whole, whole),
        out_specs=tokens, check_vma=False)
```

```python
import functools

import jax
import jax.numpy as jnp
from jax import lax
from jax.experimental import pallas as pl
from jax.experimental.pallas import tpu as pltpu
from jax.sharding import PartitionSpec as P

MESH = pl.DeviceIdType.MESH
F32, BF16 = jnp.float32, jnp.bfloat16

T, D, F, TOP = 256, 2048, 1408, 6
SLOTS, PAD, EXP = 30, 32, 4
ROWS = EXP * PAD
HALF = D // 2
PART = ((0, 88), (88, 88), (176, 80))
BIT = (4, 2, 1)
ORDER = tuple(tuple((p + i) % 3 for i in range(3)) for p in range(3))


def gather_messages(p):
    b0, b1, b2 = (BIT[d] for d in ORDER[p])
    table = ((0, 0), (0, 1), (b0, 1), (0, 2), (b0, 2), (b1, 2), (b0 | b1, 2))
    return tuple((s, i, s ^ BIT[ORDER[p][i]]) for s, i in table)


def scatter_messages(p):
    b0, b1, b2 = (BIT[d] for d in ORDER[p])
    return (
        (b0 | b1 | b2, 0, ()), (b0 | b1, 0, ()), (b0 | b2, 0, ()), (b0, 0, ()),
        (b1 | b2, 1, (0,)), (b1, 1, (1,)), (b2, 2, (2, 4)),
    )


GATHER = tuple(gather_messages(p) for p in range(3))
SCATTER = tuple(scatter_messages(p) for p in range(3))
LAST = (3, 5, 6)
WA, WB, WT = 768, 512, 128


def kernel(x, expert, slot, gate, wg, wu, wd, sg, su, sd, y, xg, *scratch):
    (ga, ua, gb, ub, gu, d0, d1, z, extra, ob, dr, r0, r1, r2, s0, s1, s2, acc, xt, comb, h, mt,
     wsem, xsem, xs_s, xs_r, meta_s, meta_r, ag_s, ag_r, fw_s, fw_r, dr_s, dr_r, rs_s, rs_r) = scratch
    me = lax.axis_index("ep")
    c, q = me % 2, me // 2
    sib = me + 1 - 2 * c
    nbr = [me + (1 - 2 * ((me // (2 * b)) % 2)) * (2 * b) for b in BIT]
    mine = pl.ds(pl.multiple_of(c * HALF, HALF), HALF)
    theirs = pl.ds(pl.multiple_of((1 - c) * HALF, HALF), HALF)
    rbuf, sbuf = (r0, r1, r2), (s0, s1, s2)

    def remote(src, dst, send, recv, to):
        return pltpu.make_async_remote_copy(
            src_ref=src, dst_ref=dst, send_sem=send, recv_sem=recv, device_id={"ep": to}, device_id_type=MESH)

    def ag(k, p, m, first=False):
        s, i, land = GATHER[p][m]
        rows = pl.ds(*PART[p])
        src = x.at[rows, mine] if first else xg.at[k, s, rows, mine]
        return remote(src, xg.at[k, land, rows, mine], ag_s.at[k, p, m], ag_r.at[k, p, m], nbr[ORDER[p][i]])

    def fwd(k, p, m):
        rows = pl.ds(*PART[p])
        piece = xg.at[k, GATHER[p][m][2], rows, mine]
        return remote(piece, piece, fw_s.at[k, p, m], fw_r.at[k, p, m], sib)

    def fwd_in(k, p, m):
        rows = pl.ds(*PART[p])
        piece = xg.at[k, GATHER[p][m][2], rows, theirs]
        return remote(piece, piece, fw_s.at[k, p, m], fw_r.at[k, p, m], sib)

    def give(k, r):
        return remote(z.at[r // 2, :, pl.ds((r % 2) * HALF, HALF)], dr.at[k, r], dr_s.at[k, r], dr_r.at[k, r], sib)

    def give_own(half):
        src = extra if half else z.at[0, :, pl.ds(0, HALF)]
        return remote(src, dr.at[half, 0], dr_s.at[half, 0], dr_r.at[half, 0], sib)

    def rs(k, p, n):
        to = nbr[ORDER[p][SCATTER[p][n][1]]]
        if n in LAST:
            return remote(sbuf[p].at[n], rbuf[p].at[c, n], rs_s.at[k, p, n], rs_r.at[c, p, n], to - c + k)
        return remote(sbuf[p].at[n], rbuf[p].at[k, n], rs_s.at[k, p, n], rs_r.at[k, p, n], to)

    def rs_in(half, p, n):
        return remote(sbuf[p].at[n], rbuf[p].at[half, n], rs_s.at[half, p, n], rs_r.at[half, p, n], sib)

    def meta_copy(i):
        return remote(mt.at[0], mt.at[i], meta_s.at[i], meta_r.at[i], xor(me, i, 4))

    def xor(v, mask, bits):
        out = v
        for b in range(bits):
            if mask >> b & 1:
                out = out + (1 - 2 * ((v // (1 << b)) % 2)) * (1 << b)
        return out

    own_send = [remote(x.at[:, cols], xg.at[c, 0, :, cols], xs_s.at[n], xs_r.at[n], sib)
                for n, cols in enumerate((theirs, mine))]
    own_recv = [remote(x.at[:, cols], xg.at[1 - c, 0, :, cols], xs_s.at[n], xs_r.at[n], sib)
                for n, cols in enumerate((mine, theirs))]
    x_in = pltpu.make_async_copy(x, xt.at[0], xsem.at[0])

    def load_a(g, u):
        return [pltpu.make_async_copy(g(0, WA), ga, wsem.at[0]), pltpu.make_async_copy(u(0, WA), ua, wsem.at[1])]

    def load_b(g, u):
        return [
            pltpu.make_async_copy(g(WA, WB), gb, wsem.at[2]),
            pltpu.make_async_copy(u(WA, WB), ub, wsem.at[3]),
            pltpu.make_async_copy(g(WA + WB, WT), gu.at[:, pl.ds(0, WT)], wsem.at[4]),
            pltpu.make_async_copy(u(WA + WB, WT), gu.at[:, pl.ds(WT, WT)], wsem.at[5]),
        ]

    def load_d(d, n):
        return [pltpu.make_async_copy(d(n * HALF, HALF), (d0, d1)[n], wsem.at[6 + n])]

    def start(copies):
        for copy in copies:
            copy.start()

    def wait(copies):
        for copy in copies:
            copy.wait()

    def routed(ref, e):
        return lambda n, w: ref.at[e, :, pl.ds(n, w)]

    def shared_in(ref, i):
        return lambda n, w: ref.at[:, pl.ds(pl.multiple_of(i * F + n, 128), w)]

    def shared_out(i):
        return lambda n, w: sd.at[pl.ds(pl.multiple_of(i * F, 128), F), pl.ds(n, w)]

    def start_gather(k):
        @pl.when(c == k)
        def _():
            for m in (0, 1, 3):
                for p in range(3):
                    ag(k, p, m, first=True).start()

        @pl.when(c != k)
        def _():
            own_recv[0].wait_recv()
            for m in (0, 1, 3):
                for p in range(3):
                    ag(k, p, m).start()

    def arrive(k, m, sends):
        for p in range(3):
            ag(k, p, m).wait_recv()
            for n in sends:
                ag(k, p, n).start()
            fwd(k, p, m).start()

    def x_load(k, r, b):
        return pltpu.make_async_copy(xg.at[k, r], xt.at[b], xsem.at[b])

    def fetch(k, r, b):
        if r:
            landed(k, r)
            x_load(k, r, b).start()
            return

        @pl.when(c == k)
        def _():
            pltpu.make_async_copy(x, xt.at[b], xsem.at[b]).start()

        @pl.when(c != k)
        def _():
            own_recv[1].wait_recv()
            x_load(k, r, b).start()

    def landed(k, r):
        for p in range(3):
            for m in range(7):
                if GATHER[p][m][2] == r:
                    fwd_in(k, p, m).wait_recv()

    def dispatch(k, r, b):
        x_load(k, r, b).wait()
        table = mt[2 * r + (k + c) % 2]
        row = (lax.broadcasted_iota(jnp.int32, (ROWS, T), 0) + me * ROWS).astype(F32)
        pick = jnp.zeros((ROWS, T), F32)
        weight = jnp.zeros((ROWS, T), F32)
        for j in range(TOP):
            hit = table[j:j + 1, :] == row
            pick = jnp.where(hit, 1.0, pick)
            weight = jnp.where(hit, table[8 + j:9 + j, :], weight)
        comb[k, r] = weight.T
        for n in range(0, D, 512):
            rows = jnp.dot(pick.astype(BF16), xt[b, :, n:n + 512], preferred_element_type=F32).astype(BF16)
            for e in range(EXP):
                z[e, r * PAD:(r + 1) * PAD, n:n + 512] = rows[e * PAD:(e + 1) * PAD]

    def gated(g, u):
        return (g * (1.0 / (1.0 + jnp.exp(-g))) * u).astype(BF16)

    def dot(a, b):
        return jnp.dot(a, b, preferred_element_type=F32)

    def hidden_a(load):
        for n in range(0, WA, 256):
            h[:, n:n + 256] = gated(dot(load(), ga[:, n:n + 256]), dot(load(), ua[:, n:n + 256]))

    def hidden_b(load):
        for n in range(0, WB, 256):
            h[:, WA + n:WA + n + 256] = gated(dot(load(), gb[:, n:n + 256]), dot(load(), ub[:, n:n + 256]))
        both = dot(load(), gu[...])
        h[:, WA + WB:] = gated(both[:, :WT], both[:, WT:])

    def down(half, store):
        for n in range(0, HALF, 512):
            store(half * HALF + n, dot(h[...], (d0, d1)[half][:, n:n + 512]))

    def give_all(k):
        for r in (7, 6, 5, 3, 4, 2, 1):
            part = dot(comb[k, r].astype(BF16), ob[k, r, :, theirs])
            z[r // 2, :, (r % 2) * HALF:(r % 2) * HALF + HALF] = part.astype(BF16)
            give(k, r).start()

        @pl.when(c != k)
        def _():
            for half in range(2):
                part = dot(comb[k, 0].astype(BF16), ob[k, 0, :, half * HALF:half * HALF + HALF]).astype(BF16)
                if half:
                    extra[...] = part
                else:
                    z[0, :, :HALF] = part
                give_own(half).start()

    def gave_all(k):
        for r in range(1, 8):
            give(k, r).wait_send()

        @pl.when(c != k)
        def _():
            for half in range(2):
                give_own(half).wait_send()

    def term(k, p, r, cols, half):
        first, rows = PART[p]
        low = first // 16 * 16
        part = dot(comb[k, r, first:first + rows, :].astype(BF16), ob[k, r, :, cols])
        other = dr[half, r, low:first + rows, :].astype(F32)[first - low:]
        return part + other

    def send_sum(k, n):
        for p in range(3):
            r, _, joins = SCATTER[p][n]
            total = term(k, p, r, mine, k)
            for j in joins:
                rs(k, p, j).wait_recv()
                total = total + rbuf[p][k, j].astype(F32)
            if k == 1:
                rs(0, p, n).wait_send()
            sbuf[p][n] = total.astype(BF16)
            rs(k, p, n).start()

    def start_scatter(k):
        give(k, 7).wait_recv()
        send_sum(k, 0)
        for r in (6, 5, 3):
            give(k, r).wait_recv()
        send_sum(k, 1)
        send_sum(k, 2)
        for r in (4, 2, 1):
            give(k, r).wait_recv()
        send_sum(k, 3)

    def finish(k):
        @pl.when(c == k)
        def _():
            for half in range(2):
                give_own(half).wait_recv()
                cols = slice(half * HALF, half * HALF + HALF)
                for p in range(3):
                    first, rows = PART[p]
                    total = term(k, p, 0, cols, half)
                    for j in LAST:
                        rs_in(half, p, j).wait_recv()
                        total = total + rbuf[p][half, j].astype(F32)
                    y[first:first + rows, cols] = (acc[first:first + rows, cols] + total).astype(BF16)

    own_send[0].start()
    x_in.start()
    start(load_a(shared_in(sg, 0), shared_in(su, 0)))
    start(load_b(shared_in(sg, 0), shared_in(su, 0)))
    for n in range(2):
        start(load_d(shared_out(0), n))
    own_send[1].start()
    for j in range(TOP):
        row = jnp.where(slot[j] < SLOTS, expert[j] * PAD + slot[j], -1).astype(F32)
        mt[0, j:j + 1, :] = row
        mt[0, 8 + j:9 + j, :] = gate[j].astype(BF16).astype(F32)
    start_gather(0)
    acc[...] = jnp.zeros_like(acc)
    for i in range(1, 16):
        meta_copy(i).start()
    x_in.wait()

    @pl.loop(0, 2)
    def _(i):
        def following(ref, routed_ref, load):
            @pl.when(i == 0)
            def _():
                start(load(*(shared_in(v, 1) for v in ref)))

            @pl.when(i == 1)
            def _():
                start(load(*(routed(v, 0) for v in routed_ref)))

        wait(load_a(shared_in(sg, i), shared_in(su, i)))
        hidden_a(lambda: xt[0])
        following((sg, su), (wg, wu), load_a)
        wait(load_b(shared_in(sg, i), shared_in(su, i)))
        hidden_b(lambda: xt[0])
        following((sg, su), (wg, wu), load_b)

        def store(n, v):
            acc[:, n:n + 512] += v

        for half in range(2):
            wait(load_d(shared_out(i), half))
            down(half, store)

            @pl.when(i == 0)
            def _():
                start(load_d(shared_out(1), half))

            @pl.when(i == 1)
            def _():
                start(load_d(routed(wd, 0), half))

        @pl.when(i == 0)
        def _():
            arrive(0, 0, (2, 4))

    arrive(0, 1, (5,))
    for i in range(1, 16):
        meta_copy(i).wait_recv()
    ORDER_IN = (0, 4, 2, 1, 6, 5, 3, 7)
    AHEAD = 2

    def dispatch_all(k, waits):
        for n in range(8 + AHEAD):
            if n < 8:
                for m in waits.get(n, ()):
                    arrive(k, m, ())
                fetch(k, ORDER_IN[n], n % (AHEAD + 1))
            if n >= AHEAD:
                dispatch(k, ORDER_IN[n - AHEAD], (n - AHEAD) % (AHEAD + 1))

    arrive(0, 2, (6,))
    start_gather(1)
    arrive(0, 3, ())
    dispatch_all(0, {4: (4, 5), 7: (6,)})

    @pl.loop(0, 8)
    def _(i):
        k, e = i // 4, i % 4
        nxt = (i + 1) % 4
        wait(load_a(routed(wg, e), routed(wu, e)))
        hidden_a(lambda: z[e])

        @pl.when(i < 7)
        def _():
            start(load_a(routed(wg, nxt), routed(wu, nxt)))

        @pl.when(i == 7)
        def _():
            send_sum(0, 6)

        wait(load_b(routed(wg, e), routed(wu, e)))
        hidden_b(lambda: z[e])

        @pl.when(i < 7)
        def _():
            start(load_b(routed(wg, nxt), routed(wu, nxt)))

        @pl.when(i == 4)
        def _():
            send_sum(0, 4)

        @pl.when(i == 5)
        def _():
            send_sum(0, 5)

        def store(n, v):
            for r in range(8):
                ob[k, r, pl.ds(pl.multiple_of(e * PAD, PAD), PAD), n:n + 512] = v[r * PAD:(r + 1) * PAD].astype(BF16)

        for half in range(2):
            wait(load_d(routed(wd, e), half))
            down(half, store)

            @pl.when(i < 7)
            def _():
                start(load_d(routed(wd, nxt), half))

        @pl.when(i == 0)
        def _():
            arrive(1, 0, (2, 4))

        @pl.when(i == 1)
        def _():
            arrive(1, 1, (5,))

        @pl.when(i == 2)
        def _():
            arrive(1, 2, (6,))
            arrive(1, 3, ())

        @pl.when(i == 3)
        def _():
            give_all(0)
            start_scatter(0)
            gave_all(0)
            dispatch_all(1, {4: (4, 5), 7: (6,)})

    give_all(1)
    start_scatter(1)
    send_sum(1, 4)
    finish(0)
    send_sum(1, 5)
    send_sum(1, 6)
    finish(1)

    for copy in own_send:
        copy.wait_send()
    for i in range(1, 16):
        meta_copy(i).wait_send()
    for k in range(2):
        for p in range(3):
            for m in range(7):
                ag(k, p, m).wait_send()
                fwd(k, p, m).wait_send()
    gave_all(1)
    for p in range(3):
        for n in range(7):
            rs(1, p, n).wait_send()


def solution(mesh):
    dma = pltpu.SemaphoreType.DMA

    def body(x, expert, slot, gate, wg, wu, wd, sg, su, sd):
        x = x.reshape(T, D)
        expert, slot, gate = (v.transpose(0, 3, 1, 2).reshape(TOP, 1, T) for v in (expert, slot, gate))
        hbm, vmem = pl.BlockSpec(memory_space=pltpu.HBM), pl.BlockSpec(memory_space=pltpu.VMEM)
        y, _ = pl.pallas_call(
            kernel,
            name="moe",
            out_shape=(jax.ShapeDtypeStruct((T, D), BF16), jax.ShapeDtypeStruct((2, 8, T, D), BF16)),
            in_specs=[hbm, vmem, vmem, vmem, hbm, hbm, hbm, hbm, hbm, hbm],
            out_specs=(vmem, hbm),
            scratch_shapes=[
                *[pltpu.VMEM((D, n), BF16) for n in (WA, WA, WB, WB, 2 * WT)],
                *[pltpu.VMEM((F, HALF), BF16)] * 2,
                pltpu.VMEM((EXP, T, D), BF16),
                pltpu.VMEM((T, HALF), BF16),
                pltpu.VMEM((2, 8, ROWS, D), BF16),
                pltpu.VMEM((2, 8, T, HALF), BF16),
                *[pltpu.VMEM((2, 7, n, HALF), BF16) for _, n in PART],
                *[pltpu.VMEM((7, n, HALF), BF16) for _, n in PART],
                pltpu.VMEM((T, D), F32),
                pltpu.VMEM((3, T, D), BF16),
                pltpu.VMEM((2, 8, T, ROWS), F32),
                pltpu.VMEM((T, F), BF16),
                pltpu.VMEM((16, 16, T), F32),
                dma((8,)), dma((3,)), dma((2,)), dma((2,)), dma((16,)), dma((16,)),
                dma((2, 3, 7)), dma((2, 3, 7)), dma((2, 3, 7)), dma((2, 3, 7)),
                dma((2, 8)), dma((2, 8)), dma((2, 3, 7)), dma((2, 3, 7)),
            ],
            compiler_params=pltpu.CompilerParams(has_side_effects=True, vmem_limit_bytes=67_043_328),
        )(x, expert, slot, gate, wg, wu, wd, sg, su, sd)
        return y.reshape(1, 1, T, D)

    tokens, experts, whole = P("dp", "ep", None, None), P("ep", None, None), P(None, None)
    return jax.shard_map(
        body, mesh=mesh,
        in_specs=(tokens, tokens, tokens, tokens, experts, experts, experts, whole, whole, whole),
        out_specs=tokens, check_vma=False)
```

```python
import functools

import jax
import jax.numpy as jnp
from jax import lax
from jax.experimental import pallas as pl
from jax.experimental.pallas import tpu as pltpu
from jax.sharding import PartitionSpec as P

MESH = pl.DeviceIdType.MESH
F32, BF16 = jnp.float32, jnp.bfloat16

T, D, F, TOP = 256, 2048, 1408, 6
SLOTS, PAD, EXP = 30, 32, 4
ROWS = EXP * PAD
HALF = D // 2
PART = ((0, 88), (88, 88), (176, 80))
BIT = (4, 2, 1)
ORDER = tuple(tuple((p + i) % 3 for i in range(3)) for p in range(3))


def gather_messages(p):
    b0, b1, b2 = (BIT[d] for d in ORDER[p])
    table = ((0, 0), (0, 1), (b0, 1), (0, 2), (b0, 2), (b1, 2), (b0 | b1, 2))
    return tuple((s, i, s ^ BIT[ORDER[p][i]]) for s, i in table)


def scatter_messages(p):
    b0, b1, b2 = (BIT[d] for d in ORDER[p])
    return (
        (b0 | b1 | b2, 0, ()), (b0 | b1, 0, ()), (b0 | b2, 0, ()), (b0, 0, ()),
        (b1 | b2, 1, (0,)), (b1, 1, (1,)), (b2, 2, (2, 4)),
    )


GATHER = tuple(gather_messages(p) for p in range(3))
SCATTER = tuple(scatter_messages(p) for p in range(3))
LAST = (3, 5, 6)
WA, WB, WT = 768, 512, 128


def kernel(x, expert, slot, gate, wg, wu, wd, sg, su, sd, y, xg, *scratch):
    (ga, ua, gb, ub, gu, d0, d1, z, ds, ob, dr, r0, r1, r2, s0, s1, s2, acc, xt, comb, h, mt, own, flat, ev, sv, gv,
     wsem, xsem, ysem, tsem, xs_s, xs_r, meta_s, meta_r, ag_s, ag_r, fw_s, fw_r, dr_s, dr_r, rs_s, rs_r) = scratch
    me = lax.axis_index("ep")
    c, q = me % 2, me // 2
    sib = me + 1 - 2 * c
    nbr = [me + (1 - 2 * ((me // (2 * b)) % 2)) * (2 * b) for b in BIT]
    mine = pl.ds(pl.multiple_of(c * HALF, HALF), HALF)
    theirs = pl.ds(pl.multiple_of((1 - c) * HALF, HALF), HALF)
    rbuf, sbuf = (r0, r1, r2), (s0, s1, s2)

    def remote(src, dst, send, recv, to):
        return pltpu.make_async_remote_copy(
            src_ref=src, dst_ref=dst, send_sem=send, recv_sem=recv, device_id={"ep": to}, device_id_type=MESH)

    def ag(k, p, m, first=False):
        s, i, land = GATHER[p][m]
        rows = pl.ds(*PART[p])
        src = x.at[rows, mine] if first else xg.at[k, s, rows, mine]
        return remote(src, xg.at[k, land, rows, mine], ag_s.at[k, p, m], ag_r.at[k, p, m], nbr[ORDER[p][i]])

    def fwd(k, p, m):
        rows = pl.ds(*PART[p])
        piece = xg.at[k, GATHER[p][m][2], rows, mine]
        return remote(piece, piece, fw_s.at[k, p, m], fw_r.at[k, p, m], sib)

    def fwd_in(k, p, m):
        rows = pl.ds(*PART[p])
        piece = xg.at[k, GATHER[p][m][2], rows, theirs]
        return remote(piece, piece, fw_s.at[k, p, m], fw_r.at[k, p, m], sib)

    def give(k, r):
        return remote(ds.at[r], dr.at[k, r], dr_s.at[k, r], dr_r.at[k, r], sib)

    def give_own(half):
        return remote(ds.at[8 * half], dr.at[half, 0], dr_s.at[half, 0], dr_r.at[half, 0], sib)

    def rs(k, p, n):
        to = nbr[ORDER[p][SCATTER[p][n][1]]]
        if n in LAST:
            return remote(sbuf[p].at[n], rbuf[p].at[c, n], rs_s.at[k, p, n], rs_r.at[c, p, n], to - c + k)
        return remote(sbuf[p].at[n], rbuf[p].at[k, n], rs_s.at[k, p, n], rs_r.at[k, p, n], to)

    def rs_in(half, p, n):
        return remote(sbuf[p].at[n], rbuf[p].at[half, n], rs_s.at[half, p, n], rs_r.at[half, p, n], sib)

    def meta_copy(i):
        return remote(own.at[i], mt.at[i], meta_s.at[i], meta_r.at[i], xor(me, i, 4))

    def xor(v, mask, bits):
        out = v
        for b in range(bits):
            if mask >> b & 1:
                out = out + (1 - 2 * ((v // (1 << b)) % 2)) * (1 << b)
        return out

    own_send = [remote(x.at[:, cols], xg.at[c, 0, :, cols], xs_s.at[n], xs_r.at[n], sib)
                for n, cols in enumerate((theirs, mine))]
    own_recv = [remote(x.at[:, cols], xg.at[1 - c, 0, :, cols], xs_s.at[n], xs_r.at[n], sib)
                for n, cols in enumerate((mine, theirs))]
    x_in = pltpu.make_async_copy(x, xt.at[0], xsem.at[0])

    def load_a(g, u):
        return [pltpu.make_async_copy(g(0, WA), ga, wsem.at[0]), pltpu.make_async_copy(u(0, WA), ua, wsem.at[1])]

    def load_b(g, u):
        return [
            pltpu.make_async_copy(g(WA, WB), gb, wsem.at[2]),
            pltpu.make_async_copy(u(WA, WB), ub, wsem.at[3]),
            pltpu.make_async_copy(g(WA + WB, WT), gu.at[:, pl.ds(0, WT)], wsem.at[4]),
            pltpu.make_async_copy(u(WA + WB, WT), gu.at[:, pl.ds(WT, WT)], wsem.at[5]),
        ]

    def load_d(d, n):
        return [pltpu.make_async_copy(d(n * HALF, HALF), (d0, d1)[n], wsem.at[6 + n])]

    def start(copies):
        for copy in copies:
            copy.start()

    def wait(copies):
        for copy in copies:
            copy.wait()

    def routed(ref, e):
        return lambda n, w: ref.at[e, :, pl.ds(n, w)]

    def shared_in(ref, i):
        return lambda n, w: ref.at[:, pl.ds(pl.multiple_of(i * F + n, 128), w)]

    def shared_out(i):
        return lambda n, w: sd.at[pl.ds(pl.multiple_of(i * F, 128), F), pl.ds(n, w)]

    def start_gather(k):
        @pl.when(c == k)
        def _():
            for m in (0, 1, 3):
                for p in range(3):
                    ag(k, p, m, first=True).start()

        @pl.when(c != k)
        def _():
            own_recv[0].wait_recv()
            for m in (0, 1, 3):
                for p in range(3):
                    ag(k, p, m).start()

    def arrive(k, m, sends):
        for p in range(3):
            ag(k, p, m).wait_recv()
            for n in sends[:1]:
                ag(k, p, n).start()
            fwd(k, p, m).start()
        for p in range(3):
            for n in sends[1:]:
                ag(k, p, n).start()

    def x_load(k, r, b):
        return pltpu.make_async_copy(xg.at[k, r], xt.at[b], xsem.at[b])

    def fetch(k, r, b):
        if r:
            landed(k, r)
            x_load(k, r, b).start()
            return

        @pl.when(c == k)
        def _():
            pltpu.make_async_copy(x, xt.at[b], xsem.at[b]).start()

        @pl.when(c != k)
        def _():
            own_recv[1].wait_recv()
            x_load(k, r, b).start()

    def landed(k, r):
        for p in range(3):
            for m in range(7):
                if GATHER[p][m][2] == r:
                    fwd_in(k, p, m).wait_recv()

    def dispatch(k, r, b):
        x_load(k, r, b).wait()
        table = mt[2 * r + (k + c) % 2].astype(F32)
        row = lax.broadcasted_iota(jnp.int32, (ROWS, T), 0).astype(F32)
        pick = jnp.zeros((ROWS, T), F32)
        weight = jnp.zeros((ROWS, T), F32)
        for j in range(TOP):
            hit = table[j:j + 1, :] == row
            pick = jnp.where(hit, 1.0, pick)
            weight = jnp.where(hit, table[8 + j:9 + j, :], weight)
        comb[k, r] = weight.T
        for n in range(0, D, 512):
            rows = jnp.dot(pick.astype(BF16), xt[b, :, n:n + 512], preferred_element_type=F32).astype(BF16)
            for e in range(EXP):
                z[e, r * PAD:(r + 1) * PAD, n:n + 512] = rows[e * PAD:(e + 1) * PAD]

    def gated(g, u):
        return (g * (1.0 / (1.0 + jnp.exp(-g))) * u).astype(BF16)

    def dot(a, b):
        return jnp.dot(a, b, preferred_element_type=F32)

    def hidden_a(load):
        for n in range(0, WA, 256):
            h[:, n:n + 256] = gated(dot(load(), ga[:, n:n + 256]), dot(load(), ua[:, n:n + 256]))

    def hidden_b(load):
        for n in range(0, WB, 256):
            h[:, WA + n:WA + n + 256] = gated(dot(load(), gb[:, n:n + 256]), dot(load(), ub[:, n:n + 256]))
        both = dot(load(), gu[...])
        h[:, WA + WB:] = gated(both[:, :WT], both[:, WT:])

    def down(half, store):
        for n in range(0, HALF, 512):
            store(half * HALF + n, dot(h[...], (d0, d1)[half][:, n:n + 512]))

    def give_all(k):
        for r in (7, 6, 5, 3, 4, 2, 1):
            part = dot(comb[k, r].astype(BF16), ob[k, r, :, theirs])
            ds[r] = part.astype(BF16)
            give(k, r).start()

        @pl.when(c != k)
        def _():
            for half in range(2):
                part = dot(comb[k, 0].astype(BF16), ob[k, 0, :, half * HALF:half * HALF + HALF])
                ds[8 * half] = part.astype(BF16)
                give_own(half).start()

    def gave_all(k):
        for r in range(1, 8):
            give(k, r).wait_send()

        @pl.when(c != k)
        def _():
            for half in range(2):
                give_own(half).wait_send()

    def term(k, p, r, cols, half):
        first, rows = PART[p]
        low = first // 16 * 16
        part = dot(comb[k, r, first:first + rows, :].astype(BF16), ob[k, r, :, cols])
        other = dr[half, r, low:first + rows, :].astype(F32)[first - low:]
        return part + other

    def send_sum(k, n):
        for p in range(3):
            r, _, joins = SCATTER[p][n]
            total = term(k, p, r, mine, k)
            for j in joins:
                rs(k, p, j).wait_recv()
                total = total + rbuf[p][k, j].astype(F32)
            if k == 1:
                rs(0, p, n).wait_send()
            sbuf[p][n] = total.astype(BF16)
            rs(k, p, n).start()

    def scatter(k, rows, messages):
        for r in rows:
            give(k, r).wait_recv()
        for n in messages:
            send_sum(k, n)

    def finish(k):
        @pl.when(c == k)
        def _():
            for half in range(2):
                give_own(half).wait_recv()
                cols = slice(half * HALF, half * HALF + HALF)
                for p in range(3):
                    first, rows = PART[p]
                    total = term(k, p, 0, cols, half)
                    for j in LAST:
                        rs_in(half, p, j).wait_recv()
                        total = total + rbuf[p][half, j].astype(F32)
                    xt[0, first:first + rows, cols] = (acc[first:first + rows, cols] + total).astype(BF16)
                result(half).start()

    def result(half):
        cols = pl.ds(half * HALF, HALF)
        return pltpu.make_async_copy(xt.at[0, :, cols], y.at[:, cols], ysem.at[half])

    tables = [pltpu.make_async_copy(a, b, tsem.at[n]) for n, (a, b) in enumerate(((expert, ev), (slot, sv), (gate, gv)))]
    start(tables)
    x_in.start()
    start(load_a(shared_in(sg, 0), shared_in(su, 0)))
    barrier = pltpu.get_barrier_semaphore()
    for i in range(1, 16):
        pl.semaphore_signal(barrier, inc=1, device_id={"ep": xor(me, i, 4)}, device_id_type=MESH)
    pl.semaphore_wait(barrier, 15)
    own_send[0].start()
    own_send[1].start()
    start_gather(0)
    start(load_b(shared_in(sg, 0), shared_in(su, 0)))
    for n in range(2):
        start(load_d(shared_out(0), n))

    wait(tables)
    flat[...] = jnp.full_like(flat, -1)
    for j in range(TOP):
        flat[j:j + 1, :] = jnp.where(sv[j] < SLOTS, ev[j] * PAD + sv[j], -1)
    gates = jnp.concatenate([gv[j] for j in range(TOP)] + [jnp.zeros((2, T), F32)], axis=0)
    for i in range(16):
        row = flat[...] - xor(me, i, 4) * ROWS
        row = jnp.where((row >= 0) & (row < ROWS), row, -1).astype(F32)
        own[i] = jnp.concatenate([row, gates], axis=0).astype(BF16)
    mt[0] = own[0]
    acc[...] = jnp.zeros_like(acc)
    for i in range(1, 16):
        meta_copy(i).start()
    x_in.wait()

    @pl.loop(0, 2)
    def _(i):
        def following(ref, routed_ref, load):
            @pl.when(i == 0)
            def _():
                start(load(*(shared_in(v, 1) for v in ref)))

            @pl.when(i == 1)
            def _():
                start(load(*(routed(v, 0) for v in routed_ref)))

        wait(load_a(shared_in(sg, i), shared_in(su, i)))
        hidden_a(lambda: xt[0])
        following((sg, su), (wg, wu), load_a)
        wait(load_b(shared_in(sg, i), shared_in(su, i)))
        hidden_b(lambda: xt[0])
        following((sg, su), (wg, wu), load_b)

        def store(n, v):
            acc[:, n:n + 512] += v

        for half in range(2):
            wait(load_d(shared_out(i), half))
            down(half, store)

            @pl.when(i == 0)
            def _():
                start(load_d(shared_out(1), half))

            @pl.when(i == 1)
            def _():
                start(load_d(routed(wd, 0), half))

        @pl.when(i == 0)
        def _():
            arrive(0, 0, (2, 4))

    arrive(0, 1, (5,))
    arrive(0, 3, ())
    for i in range(1, 16):
        meta_copy(i).wait_recv()
    ORDER_IN = (0, 4, 2, 1, 6, 5, 3, 7)
    BUFFERS = 3

    def fetch_first(k):
        for n in range(BUFFERS):
            fetch(k, ORDER_IN[n], n)

    def dispatch_all(k, events):
        for n in range(8):
            dispatch(k, ORDER_IN[n], n % BUFFERS)
            for event in events.get(n, ()):
                event()
            if n + BUFFERS < 8:
                fetch(k, ORDER_IN[n + BUFFERS], n % BUFFERS)

    fetch(0, 0, 0)
    fetch(0, 4, 1)
    arrive(0, 2, (6,))
    start_gather(1)
    fetch(0, 2, 2)
    dispatch_all(0, {1: [lambda: arrive(0, 4, ()), lambda: arrive(0, 5, ())], 4: [lambda: arrive(0, 6, ())]})

    @pl.loop(0, 8)
    def _(i):
        k, e = i // 4, i % 4
        nxt = (i + 1) % 4
        wait(load_a(routed(wg, e), routed(wu, e)))
        hidden_a(lambda: z[e])

        @pl.when(i < 7)
        def _():
            start(load_a(routed(wg, nxt), routed(wu, nxt)))

        @pl.when(i == 7)
        def _():
            send_sum(0, 6)

        wait(load_b(routed(wg, e), routed(wu, e)))
        hidden_b(lambda: z[e])

        @pl.when(i < 7)
        def _():
            start(load_b(routed(wg, nxt), routed(wu, nxt)))

        @pl.when(i == 3)
        def _():
            arrive(1, 4, ())

        @pl.when(i == 4)
        def _():
            send_sum(0, 4)

        @pl.when(i == 5)
        def _():
            send_sum(0, 5)

        def store(n, v):
            for r in range(8):
                ob[k, r, pl.ds(pl.multiple_of(e * PAD, PAD), PAD), n:n + 512] = v[r * PAD:(r + 1) * PAD].astype(BF16)

        for half in range(2):
            wait(load_d(routed(wd, e), half))
            down(half, store)

            @pl.when(i < 7)
            def _():
                start(load_d(routed(wd, nxt), half))

        @pl.when(i == 0)
        def _():
            arrive(1, 0, (2, 4))

        @pl.when(i == 1)
        def _():
            arrive(1, 1, (5,))

        @pl.when(i == 2)
        def _():
            arrive(1, 2, (6,))
            arrive(1, 3, ())

        @pl.when(i == 3)
        def _():
            arrive(1, 5, ())
            fetch_first(1)
            give_all(0)
            arrive(1, 6, ())
            scatter(0, (7,), (0,))
            dispatch_all(1, {
                3: [lambda: scatter(0, (6, 5, 3), (1, 2))],
                6: [lambda: scatter(0, (4, 2, 1), (3,))],
            })

    gave_all(0)
    give_all(1)
    scatter(1, (7,), (0,))
    scatter(1, (6, 5, 3), (1, 2))
    scatter(1, (4, 2, 1), (3,))
    send_sum(1, 4)
    finish(0)
    send_sum(1, 5)
    send_sum(1, 6)
    finish(1)

    for half in range(2):
        result(half).wait()

    for copy in own_send:
        copy.wait_send()
    for i in range(1, 16):
        meta_copy(i).wait_send()
    for k in range(2):
        for p in range(3):
            for m in range(7):
                ag(k, p, m).wait_send()
                fwd(k, p, m).wait_send()
    gave_all(1)
    for p in range(3):
        for n in range(7):
            rs(1, p, n).wait_send()


def solution(mesh):
    dma = pltpu.SemaphoreType.DMA

    def body(x, expert, slot, gate, wg, wu, wd, sg, su, sd):
        x = x.reshape(T, D)
        expert, slot, gate = (v.transpose(0, 3, 1, 2).reshape(TOP, 1, T) for v in (expert, slot, gate))
        hbm = pl.BlockSpec(memory_space=pltpu.HBM)
        y, _ = pl.pallas_call(
            kernel,
            name="moe",
            out_shape=(jax.ShapeDtypeStruct((T, D), BF16), jax.ShapeDtypeStruct((2, 8, T, D), BF16)),
            in_specs=[hbm, hbm, hbm, hbm, hbm, hbm, hbm, hbm, hbm, hbm],
            out_specs=(hbm, hbm),
            scratch_shapes=[
                *[pltpu.VMEM((D, n), BF16) for n in (WA, WA, WB, WB, 2 * WT)],
                *[pltpu.VMEM((F, HALF), BF16)] * 2,
                pltpu.VMEM((EXP, T, D), BF16),
                pltpu.VMEM((9, T, HALF), BF16),
                pltpu.VMEM((2, 8, ROWS, D), BF16),
                pltpu.VMEM((2, 8, T, HALF), BF16),
                *[pltpu.VMEM((2, 7, n, HALF), BF16) for _, n in PART],
                *[pltpu.VMEM((7, n, HALF), BF16) for _, n in PART],
                pltpu.VMEM((T, D), F32),
                pltpu.VMEM((3, T, D), BF16),
                pltpu.VMEM((2, 8, T, ROWS), F32),
                pltpu.VMEM((T, F), BF16),
                pltpu.VMEM((16, 16, T), BF16), pltpu.VMEM((16, 16, T), BF16), pltpu.VMEM((8, T), jnp.int32),
                pltpu.VMEM((TOP, 1, T), jnp.int32), pltpu.VMEM((TOP, 1, T), jnp.int32), pltpu.VMEM((TOP, 1, T), F32),
                dma((8,)), dma((3,)), dma((2,)), dma((3,)), dma((2,)), dma((2,)), dma((16,)), dma((16,)),
                dma((2, 3, 7)), dma((2, 3, 7)), dma((2, 3, 7)), dma((2, 3, 7)),
                dma((2, 8)), dma((2, 8)), dma((2, 3, 7)), dma((2, 3, 7)),
            ],
            compiler_params=pltpu.CompilerParams(collective_id=0, has_side_effects=True, vmem_limit_bytes=67_043_328),
        )(x, expert, slot, gate, wg, wu, wd, sg, su, sd)
        return y.reshape(1, 1, T, D)

    tokens, experts, whole = P("dp", "ep", None, None), P("ep", None, None), P(None, None)
    return jax.shard_map(
        body, mesh=mesh,
        in_specs=(tokens, tokens, tokens, tokens, experts, experts, experts, whole, whole, whole),
        out_specs=tokens, check_vma=False)
```

```python
import functools

import jax
import jax.numpy as jnp
from jax import lax
from jax.experimental import pallas as pl
from jax.experimental.pallas import tpu as pltpu
from jax.sharding import PartitionSpec as P

MESH = pl.DeviceIdType.MESH
F32, BF16 = jnp.float32, jnp.bfloat16

T, D, F, TOP = 256, 2048, 1408, 6
SLOTS, PAD, EXP = 30, 32, 4
ROWS = EXP * PAD
HALF = D // 2
PART = ((0, 88), (88, 88), (176, 80))
BIT = (4, 2, 1)
ORDER = tuple(tuple((p + i) % 3 for i in range(3)) for p in range(3))


def gather_messages(p):
    b0, b1, b2 = (BIT[d] for d in ORDER[p])
    table = ((0, 0), (0, 1), (b0, 1), (0, 2), (b0, 2), (b1, 2), (b0 | b1, 2))
    return tuple((s, i, s ^ BIT[ORDER[p][i]]) for s, i in table)


def scatter_messages(p):
    b0, b1, b2 = (BIT[d] for d in ORDER[p])
    return (
        (b0 | b1 | b2, 0, ()), (b0 | b1, 0, ()), (b0 | b2, 0, ()), (b0, 0, ()),
        (b1 | b2, 1, (0,)), (b1, 1, (1,)), (b2, 2, (2, 4)),
    )


GATHER = tuple(gather_messages(p) for p in range(3))
SCATTER = tuple(scatter_messages(p) for p in range(3))
GROUP = (None, 2, 2, 1, 2, 1, 1, 0)
LAST = (3, 5, 6)
PLACE = {0: 0, 1: 1, 2: 2, 4: 3}
WA, WB, WT = 768, 512, 128


def kernel(x, expert, slot, gate, wg, wu, wd, sg, su, sd, pt, rl, xg, *scratch):
    (ga, ua, gb, ub, gu, d0, d1, z, ds, ob, dr, r0, r1, r2, s0, s1, s2, acc, xt, comb, h, mt, own, flat, ev, sv, gv,
     wsem, xsem, psem, tsem, xs_s, xs_r, meta_s, meta_r, ag_s, ag_r, fw_s, fw_r, dr_s, dr_r, own_s, own_r, rs_s, rs_r) = scratch
    me = lax.axis_index("ep")
    c, q = me % 2, me // 2
    sib = me + 1 - 2 * c
    nbr = [me + (1 - 2 * ((me // (2 * b)) % 2)) * (2 * b) for b in BIT]
    mine = pl.ds(pl.multiple_of(c * HALF, HALF), HALF)
    theirs = pl.ds(pl.multiple_of((1 - c) * HALF, HALF), HALF)
    rbuf, sbuf = (r0, r1, r2), (s0, s1, s2)

    def remote(src, dst, send, recv, to):
        return pltpu.make_async_remote_copy(
            src_ref=src, dst_ref=dst, send_sem=send, recv_sem=recv, device_id={"ep": to}, device_id_type=MESH)

    def ag(k, p, m, first=False):
        s, i, land = GATHER[p][m]
        rows = pl.ds(*PART[p])
        src = x.at[rows, mine] if first else xg.at[k, s, rows, mine]
        return remote(src, xg.at[k, land, rows, mine], ag_s.at[k], ag_r.at[k, m], nbr[ORDER[p][i]])

    def ag_in(k, m):
        piece = xg.at[k, 0, :, mine]
        return remote(piece, piece, ag_s.at[k], ag_r.at[k, m], sib)

    def fwd(k, p, m):
        land = GATHER[p][m][2]
        piece = xg.at[k, land, pl.ds(*PART[p]), mine]
        return remote(piece, piece, fw_s.at[k], fw_r.at[k, land], sib)

    def fwd_in(k, r):
        piece = xg.at[k, r, :, theirs]
        return remote(piece, piece, fw_s.at[k], fw_r.at[k, r], sib)

    def gathered(k):
        sent = xg.at[k, pl.ds(0, 7), :, mine]
        return remote(sent, sent, ag_s.at[k], ag_r.at[k, 0], sib), remote(sent, sent, fw_s.at[k], fw_r.at[k, 0], sib)

    def give(k, r):
        return remote(ds.at[r], dr.at[k, r], dr_s.at[k], dr_r.at[k, GROUP[r]], sib)

    def give_in(k, n, g):
        return remote(ds.at[pl.ds(0, n)], dr.at[k, pl.ds(0, n)], dr_s.at[k], dr_r.at[k, g], sib)

    def give_own(half):
        return remote(ds.at[8 * half], dr.at[half, 0], own_s, own_r, sib)

    def gave_own():
        return remote(ds.at[pl.ds(0, 2)], dr.at[0, pl.ds(0, 2)], own_s, own_r, sib)

    def rs(k, p, n):
        to = nbr[ORDER[p][SCATTER[p][n][1]]]
        send = rs_s.at[k, n // 6]
        if n in LAST:
            return remote(sbuf[p].at[n], rl.at[LAST.index(n), pl.ds(*PART[p]), mine], send, rs_r.at[c, n], to - c + k)
        return remote(sbuf[p].at[n], rbuf[p].at[k, PLACE[n]], send, rs_r.at[k, n], to)

    def rs_in(k, n):
        piece = rl.at[0, :, mine]
        return remote(piece, piece, rs_s.at[k, 0], rs_r.at[k, n], sib)

    def rs_sent(k, g):
        sent = xg.at[k, pl.ds(0, 1 if g else 6), :, mine]
        return remote(sent, sent, rs_s.at[k, g], rs_r.at[k, 0], sib)

    def meta_copy(i):
        return remote(own.at[i], mt.at[i], meta_s, meta_r, xor(me, i, 4))

    def meta_all():
        return remote(own.at[pl.ds(1, 15)], mt.at[pl.ds(1, 15)], meta_s, meta_r, sib)

    def xor(v, mask, bits):
        out = v
        for b in range(bits):
            if mask >> b & 1:
                out = out + (1 - 2 * ((v // (1 << b)) % 2)) * (1 << b)
        return out

    own_send = [remote(x.at[:, cols], xg.at[c, 0, :, cols], xs_s.at[n], xs_r.at[n], sib)
                for n, cols in enumerate((theirs, mine))]
    own_recv = [remote(x.at[:, cols], xg.at[1 - c, 0, :, cols], xs_s.at[n], xs_r.at[n], sib)
                for n, cols in enumerate((mine, theirs))]
    x_in = pltpu.make_async_copy(x, xt.at[0], xsem.at[0])

    def load_a(g, u):
        return [pltpu.make_async_copy(g(0, WA), ga, wsem.at[0]), pltpu.make_async_copy(u(0, WA), ua, wsem.at[1])]

    def load_b(g, u):
        return [
            pltpu.make_async_copy(g(WA, WB), gb, wsem.at[2]),
            pltpu.make_async_copy(u(WA, WB), ub, wsem.at[3]),
            pltpu.make_async_copy(g(WA + WB, WT), gu.at[:, pl.ds(0, WT)], wsem.at[4]),
            pltpu.make_async_copy(u(WA + WB, WT), gu.at[:, pl.ds(WT, WT)], wsem.at[5]),
        ]

    def load_d(d):
        return [pltpu.make_async_copy(d(n * HALF, HALF), (d0, d1)[n], wsem.at[6 + n]) for n in range(2)]

    def start(copies):
        for copy in copies:
            copy.start()

    def wait(copies):
        for copy in copies:
            copy.wait()

    def routed(ref, e):
        return lambda n, w: ref.at[e, :, pl.ds(n, w)]

    def shared_in(ref, i):
        return lambda n, w: ref.at[:, pl.ds(pl.multiple_of(i * F + n, 128), w)]

    def shared_out(i):
        return lambda n, w: sd.at[pl.ds(pl.multiple_of(i * F, 128), F), pl.ds(n, w)]

    def start_gather(k):
        @pl.when(c == k)
        def _():
            for m in (0, 1, 3):
                for p in range(3):
                    ag(k, p, m, first=True).start()

        @pl.when(c != k)
        def _():
            own_recv[0].wait_recv()
            for m in (0, 1, 3):
                for p in range(3):
                    ag(k, p, m).start()

    def arrive(k, m, sends):
        ag_in(k, m).wait_recv()
        for n in sends:
            for p in range(3):
                ag(k, p, n).start()
        for p in range(3):
            fwd(k, p, m).start()

    def x_load(k, r, b):
        return pltpu.make_async_copy(xg.at[k, r], xt.at[b], xsem.at[b])

    def fetch(k, r, b):
        if r:
            fwd_in(k, r).wait_recv()
            x_load(k, r, b).start()
            return

        @pl.when(c == k)
        def _():
            pltpu.make_async_copy(x, xt.at[b], xsem.at[b]).start()

        @pl.when(c != k)
        def _():
            own_recv[1].wait_recv()
            x_load(k, r, b).start()

    def dispatch(k, r, b):
        x_load(k, r, b).wait()
        table = mt[2 * r + (k + c) % 2].astype(F32)
        row = lax.broadcasted_iota(jnp.int32, (ROWS, T), 0).astype(F32)
        pick = jnp.zeros((ROWS, T), F32)
        weight = jnp.zeros((ROWS, T), F32)
        for j in range(TOP):
            hit = table[j:j + 1, :] == row
            pick = jnp.where(hit, 1.0, pick)
            weight = jnp.where(hit, table[8 + j:9 + j, :], weight)
        comb[k, r] = weight.T
        for n in range(0, D, 512):
            rows = jnp.dot(pick.astype(BF16), xt[b, :, n:n + 512], preferred_element_type=F32).astype(BF16)
            for e in range(EXP):
                z[e, r * PAD:(r + 1) * PAD, n:n + 512] = rows[e * PAD:(e + 1) * PAD]

    def gated(g, u):
        return (g * (1.0 / (1.0 + jnp.exp(-g))) * u).astype(BF16)

    def dot(a, b):
        return jnp.dot(a, b, preferred_element_type=F32)

    def hidden_a(load):
        for n in range(0, WA, 256):
            h[:, n:n + 256] = gated(dot(load(), ga[:, n:n + 256]), dot(load(), ua[:, n:n + 256]))

    def hidden_b(load):
        for n in range(0, WB, 256):
            h[:, WA + n:WA + n + 256] = gated(dot(load(), gb[:, n:n + 256]), dot(load(), ub[:, n:n + 256]))
        both = dot(load(), gu[...])
        h[:, WA + WB:] = gated(both[:, :WT], both[:, WT:])

    def down(store):
        for half in range(2):
            for n in range(0, HALF, 512):
                store(half * HALF + n, dot(h[...], (d0, d1)[half][:, n:n + 512]))

    def give_some(k, rs):
        for r in rs:
            ds[r] = dot(comb[k, r].astype(BF16), ob[k, r, :, theirs]).astype(BF16)
            give(k, r).start()

    def give_owner(k):
        @pl.when(c != k)
        def _():
            for half in range(2):
                part = dot(comb[k, 0].astype(BF16), ob[k, 0, :, half * HALF:half * HALF + HALF])
                ds[8 * half] = part.astype(BF16)
                give_own(half).start()

    def gave_all(k):
        give_in(k, 7, 0).wait_send()

        @pl.when(c != k)
        def _():
            gave_own().wait_send()

    def term(k, p, r):
        first, rows = PART[p]
        low = first // 16 * 16
        part = dot(comb[k, r, first:first + rows, :].astype(BF16), ob[k, r, :, mine])
        other = dr[k, r, low:first + rows, :].astype(F32)[first - low:]
        return part + other

    def send_sum(k, n):
        for j in SCATTER[0][n][2]:
            rs_in(k, j).wait_recv()
        for p in range(3):
            r, _, joins = SCATTER[p][n]
            total = term(k, p, r)
            for j in joins:
                total = total + rbuf[p][k, PLACE[j]].astype(F32)
            sbuf[p][n] = total.astype(BF16)
            rs(k, p, n).start()

    def scatter(k, group, messages):
        give_in(k, 1 if group == 0 else 3, group).wait_recv()
        for n in messages:
            send_sum(k, n)

    def finish():
        gave_own().wait_recv()
        for half in range(2):
            cols = slice(half * HALF, half * HALF + HALF)
            acc[:, cols] += dot(comb[c, 0].astype(BF16), ob[c, 0, :, cols]) + dr[half, 0].astype(F32)
        result.start()

    result = pltpu.make_async_copy(acc, pt, psem)

    tables = [pltpu.make_async_copy(a, b, tsem.at[n]) for n, (a, b) in enumerate(((expert, ev), (slot, sv), (gate, gv)))]
    start(tables)
    x_in.start()
    start(load_a(shared_in(sg, 0), shared_in(su, 0)))
    barrier = pltpu.get_barrier_semaphore()
    for i in range(1, 16):
        pl.semaphore_signal(barrier, inc=1, device_id={"ep": xor(me, i, 4)}, device_id_type=MESH)
    pl.semaphore_wait(barrier, 15)
    own_send[0].start()
    own_send[1].start()
    start_gather(0)
    start(load_b(shared_in(sg, 0), shared_in(su, 0)))
    start(load_d(shared_out(0)))

    wait(tables)
    flat[...] = jnp.full_like(flat, -1)
    for j in range(TOP):
        flat[j:j + 1, :] = jnp.where(sv[j] < SLOTS, ev[j] * PAD + sv[j], -1)
    gates = jnp.concatenate([gv[j] for j in range(TOP)] + [jnp.zeros((2, T), F32)], axis=0)
    for i in range(16):
        row = flat[...] - xor(me, i, 4) * ROWS
        row = jnp.where((row >= 0) & (row < ROWS), row, -1).astype(F32)
        own[i] = jnp.concatenate([row, gates], axis=0).astype(BF16)
    mt[0] = own[0]
    acc[...] = jnp.zeros_like(acc)
    for i in range(1, 16):
        meta_copy(i).start()
    x_in.wait()

    @pl.loop(0, 2)
    def _(i):
        def following(ref, routed_ref, load):
            @pl.when(i == 0)
            def _():
                start(load(*(shared_in(v, 1) for v in ref)))

            @pl.when(i == 1)
            def _():
                start(load(*(routed(v, 0) for v in routed_ref)))

        wait(load_a(shared_in(sg, i), shared_in(su, i)))
        hidden_a(lambda: xt[0])
        following((sg, su), (wg, wu), load_a)
        wait(load_b(shared_in(sg, i), shared_in(su, i)))
        hidden_b(lambda: xt[0])
        following((sg, su), (wg, wu), load_b)

        def store(n, v):
            acc[:, n:n + 512] += v

        wait(load_d(shared_out(i)))
        down(store)

        @pl.when(i == 0)
        def _():
            start(load_d(shared_out(1)))

        @pl.when(i == 1)
        def _():
            start(load_d(routed(wd, 0)))

        @pl.when(i == 0)
        def _():
            arrive(0, 0, (2, 4))

    arrive(0, 1, (5,))
    arrive(0, 3, ())
    meta_all().wait_recv()
    ORDER_IN = (0, 4, 2, 1, 6, 5, 3, 7)
    BUFFERS = 3

    def run(k, steps):
        for step in steps:
            if callable(step):
                step()
            elif step > 0:
                fetch(k, ORDER_IN[step - 1], (step - 1) % BUFFERS)
            else:
                dispatch(k, ORDER_IN[-step - 1], (-step - 1) % BUFFERS)

    run(0, (1, 2, lambda: arrive(0, 2, (6,)), lambda: start_gather(1), 3, -1, 4, -2, lambda: arrive(0, 4, ()), -3, -4,
            lambda: arrive(0, 5, ()), 5, 6, 7, -5, -6, -7, lambda: arrive(0, 6, ()), 8, -8))

    @pl.loop(0, 8)
    def _(i):
        k, e = i // 4, i % 4
        nxt = (i + 1) % 4
        wait(load_a(routed(wg, e), routed(wu, e)))
        hidden_a(lambda: z[e])
        start(load_a(routed(wg, nxt), routed(wu, nxt)))
        wait(load_b(routed(wg, e), routed(wu, e)))
        hidden_b(lambda: z[e])
        start(load_b(routed(wg, nxt), routed(wu, nxt)))

        @pl.when(i == 0)
        def _():
            arrive(1, 0, (2, 4))

        @pl.when(i == 3)
        def _():
            arrive(1, 4, ())

        def store(n, v):
            for r in range(8):
                ob[k, r, pl.ds(pl.multiple_of(e * PAD, PAD), PAD), n:n + 512] = v[r * PAD:(r + 1) * PAD].astype(BF16)

        wait(load_d(routed(wd, e)))
        down(store)
        start(load_d(routed(wd, nxt)))

        @pl.when(i == 1)
        def _():
            arrive(1, 1, (5,))

        @pl.when(i == 2)
        def _():
            arrive(1, 2, (6,))
            arrive(1, 3, ())

        @pl.when(i == 3)
        def _():
            run(1, (
                1, 2, 3, lambda: arrive(1, 5, ()), lambda: give_some(0, (7, 6, 5, 3)), lambda: scatter(0, 0, (0,)),
                lambda: arrive(1, 6, ()), lambda: give_some(0, (4, 2, 1)), lambda: give_owner(0),
                -1, 4, -2, 5, -3, 6, -4, 7, lambda: scatter(0, 1, (1, 2)), -5, 8, -6, -7,
                lambda: scatter(0, 2, (3,)), -8))

        @pl.when(i == 4)
        def _():
            send_sum(0, 4)

        @pl.when(i == 5)
        def _():
            send_sum(0, 5)

        @pl.when(i == 6)
        def _():
            send_sum(0, 6)

    gave_all(0)
    give_some(1, (7, 6, 5, 3))
    rs_sent(0, 0).wait_send()
    scatter(1, 0, (0,))
    give_some(1, (4, 2, 1))
    scatter(1, 1, (1, 2))
    scatter(1, 2, (3,))
    give_owner(1)
    send_sum(1, 4)
    send_sum(1, 5)
    finish()
    wait(load_a(routed(wg, 0), routed(wu, 0)) + load_b(routed(wg, 0), routed(wu, 0)) + load_d(routed(wd, 0)))
    rs_sent(0, 1).wait_send()
    send_sum(1, 6)

    result.wait()
    for copy in own_send:
        copy.wait_send()
    meta_all().wait_send()
    for k in range(2):
        for copies in gathered(k):
            copies.wait_send()
    gave_all(1)
    for g in range(2):
        rs_sent(1, g).wait_send()
    for n in LAST:
        for half in range(2):
            rs_in(half, n).wait_recv()


def solution(mesh):
    dma = pltpu.SemaphoreType.DMA

    def body(x, expert, slot, gate, wg, wu, wd, sg, su, sd):
        x = x.reshape(T, D)
        expert, slot, gate = (v.transpose(0, 3, 1, 2).reshape(TOP, 1, T) for v in (expert, slot, gate))
        hbm = pl.BlockSpec(memory_space=pltpu.HBM)
        own, others, _ = pl.pallas_call(
            kernel,
            name="moe",
            out_shape=(
                jax.ShapeDtypeStruct((T, D), F32), jax.ShapeDtypeStruct((3, T, D), BF16),
                jax.ShapeDtypeStruct((2, 8, T, D), BF16)),
            in_specs=[hbm, hbm, hbm, hbm, hbm, hbm, hbm, hbm, hbm, hbm],
            out_specs=(hbm, hbm, hbm),
            scratch_shapes=[
                *[pltpu.VMEM((D, n), BF16) for n in (WA, WA, WB, WB, 2 * WT)],
                *[pltpu.VMEM((F, HALF), BF16)] * 2,
                pltpu.VMEM((EXP, T, D), BF16),
                pltpu.VMEM((9, T, HALF), BF16),
                pltpu.VMEM((2, 8, ROWS, D), BF16),
                pltpu.VMEM((2, 8, T, HALF), BF16),
                *[pltpu.VMEM((2, 4, n, HALF), BF16) for _, n in PART],
                *[pltpu.VMEM((7, n, HALF), BF16) for _, n in PART],
                pltpu.VMEM((T, D), F32),
                pltpu.VMEM((3, T, D), BF16),
                pltpu.VMEM((2, 8, T, ROWS), F32),
                pltpu.VMEM((T, F), BF16),
                pltpu.VMEM((16, 16, T), BF16), pltpu.VMEM((16, 16, T), BF16), pltpu.VMEM((8, T), jnp.int32),
                pltpu.VMEM((TOP, 1, T), jnp.int32), pltpu.VMEM((TOP, 1, T), jnp.int32), pltpu.VMEM((TOP, 1, T), F32),
                dma((8,)), dma((3,)), dma, dma((3,)), dma((2,)), dma((2,)), dma, dma,
                dma((2,)), dma((2, 7)), dma((2,)), dma((2, 8)), dma((2,)), dma((2, 3)), dma, dma,
                dma((2, 2)), dma((2, 7)),
            ],
            compiler_params=pltpu.CompilerParams(collective_id=0, has_side_effects=True, vmem_limit_bytes=67_043_328),
        )(x, expert, slot, gate, wg, wu, wd, sg, su, sd)
        for n in range(3):
            own = own + others[n].astype(F32)
        return own.astype(BF16).reshape(1, 1, T, D)

    tokens, experts, whole = P("dp", "ep", None, None), P("ep", None, None), P(None, None)
    return jax.shard_map(
        body, mesh=mesh,
        in_specs=(tokens, tokens, tokens, tokens, experts, experts, experts, whole, whole, whole),
        out_specs=tokens, check_vma=False)
```

```python
import functools

import jax
import jax.numpy as jnp
from jax import lax
from jax.experimental import pallas as pl
from jax.experimental.pallas import tpu as pltpu
from jax.sharding import PartitionSpec as P

MESH = pl.DeviceIdType.MESH
F32, BF16 = jnp.float32, jnp.bfloat16

T, D, F, TOP = 256, 2048, 1408, 6
SLOTS, PAD, EXP = 30, 32, 4
ROWS = EXP * PAD
HALF = D // 2
PART = ((0, 88), (88, 88), (176, 80))
BIT = (4, 2, 1)
ORDER = tuple(tuple((p + i) % 3 for i in range(3)) for p in range(3))


def gather_messages(p):
    b0, b1, b2 = (BIT[d] for d in ORDER[p])
    table = ((0, 0), (0, 1), (b0, 1), (0, 2), (b0, 2), (b1, 2), (b0 | b1, 2))
    return tuple((s, i, s ^ BIT[ORDER[p][i]]) for s, i in table)


def scatter_messages(p):
    b0, b1, b2 = (BIT[d] for d in ORDER[p])
    return (
        (b0 | b1 | b2, 0, ()), (b0 | b1, 0, ()), (b0 | b2, 0, ()), (b0, 0, ()),
        (b1 | b2, 1, (0,)), (b1, 1, (1,)), (b2, 2, (2, 4)),
    )


GATHER = tuple(gather_messages(p) for p in range(3))
SCATTER = tuple(scatter_messages(p) for p in range(3))
GROUP = (None, 2, 2, 1, 2, 1, 1, 0)
LAST = (3, 5, 6)
PLACE = {0: 0, 1: 1, 2: 2, 4: 3}
WA, WB, WT = 768, 512, 128


def kernel(x, expert, slot, gate, wg, wu, wd, sg, su, sd, pt, rl, xg, *scratch):
    (ga, ua, gb, ub, gu, d0, d1, z, ds, ob, dr, r0, r1, r2, l0, l1, l2, s0, s1, s2, acc, xt, comb, h, mt, own, flat, ev, sv, gv,
     wsem, xsem, psem, tsem, xs_s, xs_r, meta_s, meta_r, ag_s, ag_r, fw_s, fw_r, dr_s, dr_r, own_s, own_r, rs_s, rs_r) = scratch
    me = lax.axis_index("ep")
    c, q = me % 2, me // 2
    sib = me + 1 - 2 * c
    nbr = [me + (1 - 2 * ((me // (2 * b)) % 2)) * (2 * b) for b in BIT]
    mine = pl.ds(pl.multiple_of(c * HALF, HALF), HALF)
    theirs = pl.ds(pl.multiple_of((1 - c) * HALF, HALF), HALF)
    rbuf, lbuf, sbuf = (r0, r1, r2), (l0, l1, l2), (s0, s1, s2)

    def remote(src, dst, send, recv, to):
        return pltpu.make_async_remote_copy(
            src_ref=src, dst_ref=dst, send_sem=send, recv_sem=recv, device_id={"ep": to}, device_id_type=MESH)

    def ag(k, p, m, first=False):
        s, i, land = GATHER[p][m]
        rows = pl.ds(*PART[p])
        src = x.at[rows, mine] if first else xg.at[k, s, rows, mine]
        return remote(src, xg.at[k, land, rows, mine], ag_s.at[k], ag_r.at[k, m], nbr[ORDER[p][i]])

    def ag_in(k, m):
        piece = xg.at[k, 0, :, mine]
        return remote(piece, piece, ag_s.at[k], ag_r.at[k, m], sib)

    def fwd(k, p, m):
        land = GATHER[p][m][2]
        piece = xg.at[k, land, pl.ds(*PART[p]), mine]
        return remote(piece, piece, fw_s.at[k], fw_r.at[k, land], sib)

    def fwd_in(k, r):
        piece = xg.at[k, r, :, theirs]
        return remote(piece, piece, fw_s.at[k], fw_r.at[k, r], sib)

    def gathered(k):
        sent = xg.at[k, pl.ds(0, 7), :, mine]
        return remote(sent, sent, ag_s.at[k], ag_r.at[k, 0], sib), remote(sent, sent, fw_s.at[k], fw_r.at[k, 0], sib)

    def give(k, r):
        return remote(ds.at[r], dr.at[k, r], dr_s.at[k], dr_r.at[k, GROUP[r]], sib)

    def give_in(k, n, g):
        return remote(ds.at[pl.ds(0, n)], dr.at[k, pl.ds(0, n)], dr_s.at[k], dr_r.at[k, g], sib)

    def give_own(half):
        return remote(ds.at[8 * half], dr.at[half, 0], own_s, own_r, sib)

    def gave_own():
        return remote(ds.at[pl.ds(0, 2)], dr.at[0, pl.ds(0, 2)], own_s, own_r, sib)

    def rs(k, p, n):
        to = nbr[ORDER[p][SCATTER[p][n][1]]]
        send = rs_s.at[k, n // 6]
        if n in LAST:
            land = rl.at[pl.ds(*PART[p]), mine] if n == LAST[2] else lbuf[p].at[LAST.index(n), c]
            return remote(sbuf[p].at[n], land, send, rs_r.at[c, n], to - c + k)
        return remote(sbuf[p].at[n], rbuf[p].at[k, PLACE[n]], send, rs_r.at[k, n], to)

    def rs_in(k, n):
        piece = rl.at[:, mine]
        return remote(piece, piece, rs_s.at[k, 0], rs_r.at[k, n], sib)

    def rs_sent(k, g):
        sent = xg.at[k, pl.ds(0, 1 if g else 6), :, mine]
        return remote(sent, sent, rs_s.at[k, g], rs_r.at[k, 0], sib)

    def meta_copy(i):
        return remote(own.at[i], mt.at[i], meta_s, meta_r, xor(me, i, 4))

    def meta_all():
        return remote(own.at[pl.ds(1, 15)], mt.at[pl.ds(1, 15)], meta_s, meta_r, sib)

    def xor(v, mask, bits):
        out = v
        for b in range(bits):
            if mask >> b & 1:
                out = out + (1 - 2 * ((v // (1 << b)) % 2)) * (1 << b)
        return out

    own_send = [remote(x.at[:, cols], xg.at[c, 0, :, cols], xs_s.at[n], xs_r.at[n], sib)
                for n, cols in enumerate((theirs, mine))]
    own_recv = [remote(x.at[:, cols], xg.at[1 - c, 0, :, cols], xs_s.at[n], xs_r.at[n], sib)
                for n, cols in enumerate((mine, theirs))]
    x_in = pltpu.make_async_copy(x, xt.at[0], xsem.at[0])

    def load_a(g, u):
        return [pltpu.make_async_copy(g(0, WA), ga, wsem.at[0]), pltpu.make_async_copy(u(0, WA), ua, wsem.at[1])]

    def load_b(g, u):
        return [
            pltpu.make_async_copy(g(WA, WB), gb, wsem.at[2]),
            pltpu.make_async_copy(u(WA, WB), ub, wsem.at[3]),
            pltpu.make_async_copy(g(WA + WB, WT), gu.at[:, pl.ds(0, WT)], wsem.at[4]),
            pltpu.make_async_copy(u(WA + WB, WT), gu.at[:, pl.ds(WT, WT)], wsem.at[5]),
        ]

    def load_d(d):
        return [pltpu.make_async_copy(d(n * HALF, HALF), (d0, d1)[n], wsem.at[6 + n]) for n in range(2)]

    def start(copies):
        for copy in copies:
            copy.start()

    def wait(copies):
        for copy in copies:
            copy.wait()

    def routed(ref, e):
        return lambda n, w: ref.at[e, :, pl.ds(n, w)]

    def shared_in(ref, i):
        return lambda n, w: ref.at[:, pl.ds(pl.multiple_of(i * F + n, 128), w)]

    def shared_out(i):
        return lambda n, w: sd.at[pl.ds(pl.multiple_of(i * F, 128), F), pl.ds(n, w)]

    def start_gather(k):
        @pl.when(c == k)
        def _():
            for m in (0, 1, 3):
                for p in range(3):
                    ag(k, p, m, first=True).start()

        @pl.when(c != k)
        def _():
            own_recv[0].wait_recv()
            for m in (0, 1, 3):
                for p in range(3):
                    ag(k, p, m).start()

    def arrive(k, m, sends):
        ag_in(k, m).wait_recv()
        for n in sends:
            for p in range(3):
                ag(k, p, n).start()
        for p in range(3):
            fwd(k, p, m).start()

    def x_load(k, r, b):
        return pltpu.make_async_copy(xg.at[k, r], xt.at[b], xsem.at[b])

    def fetch(k, r, b):
        if r:
            fwd_in(k, r).wait_recv()
            x_load(k, r, b).start()
            return

        @pl.when(c == k)
        def _():
            pltpu.make_async_copy(x, xt.at[b], xsem.at[b]).start()

        @pl.when(c != k)
        def _():
            own_recv[1].wait_recv()
            x_load(k, r, b).start()

    def dispatch(k, r, b):
        x_load(k, r, b).wait()
        table = mt[2 * r + (k + c) % 2].astype(F32)
        row = lax.broadcasted_iota(jnp.int32, (ROWS, T), 0).astype(F32)
        pick = jnp.zeros((ROWS, T), F32)
        weight = jnp.zeros((ROWS, T), F32)
        for j in range(TOP):
            hit = table[j:j + 1, :] == row
            pick = jnp.where(hit, 1.0, pick)
            weight = jnp.where(hit, table[8 + j:9 + j, :], weight)
        comb[k, r] = weight.T
        for n in range(0, D, 512):
            rows = jnp.dot(pick.astype(BF16), xt[b, :, n:n + 512], preferred_element_type=F32).astype(BF16)
            for e in range(EXP):
                z[e, r * PAD:(r + 1) * PAD, n:n + 512] = rows[e * PAD:(e + 1) * PAD]

    def gated(g, u):
        return (g * (1.0 / (1.0 + jnp.exp(-g))) * u).astype(BF16)

    def dot(a, b):
        return jnp.dot(a, b, preferred_element_type=F32)

    def hidden_a(load):
        for n in range(0, WA, 256):
            h[:, n:n + 256] = gated(dot(load(), ga[:, n:n + 256]), dot(load(), ua[:, n:n + 256]))

    def hidden_b(load):
        for n in range(0, WB, 256):
            h[:, WA + n:WA + n + 256] = gated(dot(load(), gb[:, n:n + 256]), dot(load(), ub[:, n:n + 256]))
        both = dot(load(), gu[...])
        h[:, WA + WB:] = gated(both[:, :WT], both[:, WT:])

    def down(store, halves=(0, 1)):
        for half in halves:
            for n in range(0, HALF, 512):
                store(half * HALF + n, dot(h[...], (d0, d1)[half][:, n:n + 512]))

    def give_some(k, rs):
        for r in rs:
            ds[r] = dot(comb[k, r].astype(BF16), ob[k, r, :, theirs]).astype(BF16)
            give(k, r).start()

    def give_owner(k):
        @pl.when(c != k)
        def _():
            for half in range(2):
                part = dot(comb[k, 0].astype(BF16), ob[k, 0, :, half * HALF:half * HALF + HALF])
                ds[8 * half] = part.astype(BF16)
                give_own(half).start()

    def gave_all(k):
        give_in(k, 7, 0).wait_send()

        @pl.when(c != k)
        def _():
            gave_own().wait_send()

    def term(k, p, r):
        first, rows = PART[p]
        low = first // 16 * 16
        part = dot(comb[k, r, first:first + rows, :].astype(BF16), ob[k, r, :, mine])
        other = dr[k, r, low:first + rows, :].astype(F32)[first - low:]
        return part + other

    def send_sum(k, n):
        for j in SCATTER[0][n][2]:
            rs_in(k, j).wait_recv()
        for p in range(3):
            r, _, joins = SCATTER[p][n]
            total = term(k, p, r)
            for j in joins:
                total = total + rbuf[p][k, PLACE[j]].astype(F32)
            sbuf[p][n] = total.astype(BF16)
            rs(k, p, n).start()

    def scatter(k, group, messages):
        give_in(k, 1 if group == 0 else 3, group).wait_recv()
        for n in messages:
            send_sum(k, n)

    def finish():
        gave_own().wait_recv()
        for half in range(2):
            cols = slice(half * HALF, half * HALF + HALF)
            acc[:, cols] += dot(comb[c, 0].astype(BF16), ob[c, 0, :, cols]) + dr[half, 0].astype(F32)

    def finish_arrived():
        for n in range(2):
            for half in range(2):
                rs_in(half, LAST[n]).wait_recv()
        for half in range(2):
            cols = slice(half * HALF, half * HALF + HALF)
            for p in range(3):
                first, rows = PART[p]
                acc[first:first + rows, cols] += lbuf[p][0, half].astype(F32) + lbuf[p][1, half].astype(F32)
        result.start()

    result = pltpu.make_async_copy(acc, pt, psem)

    tables = [pltpu.make_async_copy(a, b, tsem.at[n]) for n, (a, b) in enumerate(((expert, ev), (slot, sv), (gate, gv)))]
    start(tables)
    x_in.start()
    start(load_a(shared_in(sg, 0), shared_in(su, 0)))
    barrier = pltpu.get_barrier_semaphore()
    for i in range(1, 16):
        pl.semaphore_signal(barrier, inc=1, device_id={"ep": xor(me, i, 4)}, device_id_type=MESH)
    pl.semaphore_wait(barrier, 15)
    own_send[0].start()
    own_send[1].start()
    start_gather(0)
    start(load_b(shared_in(sg, 0), shared_in(su, 0)))
    start(load_d(shared_out(0)))

    wait(tables)
    flat[...] = jnp.full_like(flat, -1)
    for j in range(TOP):
        flat[j:j + 1, :] = jnp.where(sv[j] < SLOTS, ev[j] * PAD + sv[j], -1)
    gates = jnp.concatenate([gv[j] for j in range(TOP)] + [jnp.zeros((2, T), F32)], axis=0)
    for i in range(16):
        row = flat[...] - xor(me, i, 4) * ROWS
        row = jnp.where((row >= 0) & (row < ROWS), row, -1).astype(F32)
        own[i] = jnp.concatenate([row, gates], axis=0).astype(BF16)
    mt[0] = own[0]
    acc[...] = jnp.zeros_like(acc)
    for i in range(1, 16):
        meta_copy(i).start()
    x_in.wait()

    @pl.loop(0, 2)
    def _(i):
        def following(ref, routed_ref, load):
            @pl.when(i == 0)
            def _():
                start(load(*(shared_in(v, 1) for v in ref)))

            @pl.when(i == 1)
            def _():
                start(load(*(routed(v, 0) for v in routed_ref)))

        wait(load_a(shared_in(sg, i), shared_in(su, i)))
        hidden_a(lambda: xt[0])
        following((sg, su), (wg, wu), load_a)
        wait(load_b(shared_in(sg, i), shared_in(su, i)))
        hidden_b(lambda: xt[0])
        following((sg, su), (wg, wu), load_b)

        def store(n, v):
            acc[:, n:n + 512] += v

        wait(load_d(shared_out(i)))
        down(store)

        @pl.when(i == 0)
        def _():
            start(load_d(shared_out(1)))

        @pl.when(i == 1)
        def _():
            start(load_d(routed(wd, 0)))

        @pl.when(i == 0)
        def _():
            arrive(0, 0, (2, 4))

    arrive(0, 1, (5,))
    arrive(0, 3, ())
    meta_all().wait_recv()
    ORDER_IN = (0, 4, 2, 1, 6, 5, 3, 7)
    BUFFERS = 3

    def run(k, steps):
        for step in steps:
            if callable(step):
                step()
            elif step > 0:
                fetch(k, ORDER_IN[step - 1], (step - 1) % BUFFERS)
            else:
                dispatch(k, ORDER_IN[-step - 1], (-step - 1) % BUFFERS)

    run(0, (1, 2, lambda: arrive(0, 2, (6,)), lambda: start_gather(1), 3, -1, 4, -2, lambda: arrive(0, 4, ()), -3, -4,
            lambda: arrive(0, 5, ()), 5, 6, 7, -5, -6, -7, lambda: arrive(0, 6, ()), 8, -8))

    @pl.loop(0, 8)
    def _(i):
        k, e = i // 4, i % 4
        nxt = (i + 1) % 4
        wait(load_a(routed(wg, e), routed(wu, e)))
        hidden_a(lambda: z[e])
        @pl.when(i < 7)
        def _():
            start(load_a(routed(wg, nxt), routed(wu, nxt)))

        @pl.when(i == 7)
        def _():
            send_sum(0, 6)

        wait(load_b(routed(wg, e), routed(wu, e)))
        hidden_b(lambda: z[e])

        @pl.when(i < 7)
        def _():
            start(load_b(routed(wg, nxt), routed(wu, nxt)))

        @pl.when(i == 0)
        def _():
            arrive(1, 0, (2, 4))

        @pl.when(i == 3)
        def _():
            arrive(1, 4, ())
            run(1, (1, 2, 3))

        @pl.when(i == 4)
        def _():
            send_sum(0, 4)

        @pl.when(i == 5)
        def _():
            send_sum(0, 5)

        def store(n, v):
            for r in range(8):
                ob[k, r, pl.ds(pl.multiple_of(e * PAD, PAD), PAD), n:n + 512] = v[r * PAD:(r + 1) * PAD].astype(BF16)

        for half in range(2):
            wait(load_d(routed(wd, e))[half:half + 1])
            down(store, (half,))

            @pl.when(i < 7)
            def _():
                start(load_d(routed(wd, nxt))[half:half + 1])

        @pl.when(i == 1)
        def _():
            arrive(1, 1, (5,))

        @pl.when(i == 2)
        def _():
            arrive(1, 2, (6,))
            arrive(1, 3, ())

        @pl.when(i == 3)
        def _():
            run(1, (
                lambda: arrive(1, 5, ()), lambda: give_some(0, (7, 6, 5, 3)), lambda: arrive(1, 6, ()),
                -1, 4, -2, 5, lambda: scatter(0, 0, (0,)), lambda: give_some(0, (4, 2, 1)), lambda: give_owner(0),
                -3, 6, -4, 7, lambda: scatter(0, 1, (1, 2)), -5, 8, -6, -7,
                lambda: scatter(0, 2, (3,)), -8))


    gave_all(0)
    give_some(1, (7, 6, 5, 3))
    rs_sent(0, 0).wait_send()
    scatter(1, 0, (0,))
    give_some(1, (4, 2, 1))
    scatter(1, 1, (1, 2))
    scatter(1, 2, (3,))
    give_owner(1)
    send_sum(1, 4)
    send_sum(1, 5)
    finish()
    rs_sent(0, 1).wait_send()
    send_sum(1, 6)
    finish_arrived()

    result.wait()
    for copy in own_send:
        copy.wait_send()
    meta_all().wait_send()
    for k in range(2):
        for copies in gathered(k):
            copies.wait_send()
    gave_all(1)
    for g in range(2):
        rs_sent(1, g).wait_send()
    for half in range(2):
        rs_in(half, LAST[2]).wait_recv()


def solution(mesh):
    dma = pltpu.SemaphoreType.DMA

    def body(x, expert, slot, gate, wg, wu, wd, sg, su, sd):
        x = x.reshape(T, D)
        expert, slot, gate = (v.transpose(0, 3, 1, 2).reshape(TOP, 1, T) for v in (expert, slot, gate))
        hbm = pl.BlockSpec(memory_space=pltpu.HBM)
        own, others, _ = pl.pallas_call(
            kernel,
            name="moe",
            out_shape=(
                jax.ShapeDtypeStruct((T, D), F32), jax.ShapeDtypeStruct((T, D), BF16),
                jax.ShapeDtypeStruct((2, 8, T, D), BF16)),
            in_specs=[hbm, hbm, hbm, hbm, hbm, hbm, hbm, hbm, hbm, hbm],
            out_specs=(hbm, hbm, hbm),
            scratch_shapes=[
                *[pltpu.VMEM((D, n), BF16) for n in (WA, WA, WB, WB, 2 * WT)],
                *[pltpu.VMEM((F, HALF), BF16)] * 2,
                pltpu.VMEM((EXP, T, D), BF16),
                pltpu.VMEM((9, T, HALF), BF16),
                pltpu.VMEM((2, 8, ROWS, D), BF16),
                pltpu.VMEM((2, 8, T, HALF), BF16),
                *[pltpu.VMEM((2, 4, n, HALF), BF16) for _, n in PART],
                *[pltpu.VMEM((2, 2, n, HALF), BF16) for _, n in PART],
                *[pltpu.VMEM((7, n, HALF), BF16) for _, n in PART],
                pltpu.VMEM((T, D), F32),
                pltpu.VMEM((3, T, D), BF16),
                pltpu.VMEM((2, 8, T, ROWS), F32),
                pltpu.VMEM((T, F), BF16),
                pltpu.VMEM((16, 16, T), BF16), pltpu.VMEM((16, 16, T), BF16), pltpu.VMEM((8, T), jnp.int32),
                pltpu.VMEM((TOP, 1, T), jnp.int32), pltpu.VMEM((TOP, 1, T), jnp.int32), pltpu.VMEM((TOP, 1, T), F32),
                dma((8,)), dma((3,)), dma, dma((3,)), dma((2,)), dma((2,)), dma, dma,
                dma((2,)), dma((2, 7)), dma((2,)), dma((2, 8)), dma((2,)), dma((2, 3)), dma, dma,
                dma((2, 2)), dma((2, 7)),
            ],
            compiler_params=pltpu.CompilerParams(collective_id=0, has_side_effects=True, vmem_limit_bytes=67_043_328),
        )(x, expert, slot, gate, wg, wu, wd, sg, su, sd)
        return (own + others.astype(F32)).astype(BF16).reshape(1, 1, T, D)

    tokens, experts, whole = P("dp", "ep", None, None), P("ep", None, None), P(None, None)
    return jax.shard_map(
        body, mesh=mesh,
        in_specs=(tokens, tokens, tokens, tokens, experts, experts, experts, whole, whole, whole),
        out_specs=tokens, check_vma=False)
```

```python
import functools

import jax
import jax.numpy as jnp
from jax import lax
from jax.experimental import pallas as pl
from jax.experimental.pallas import tpu as pltpu
from jax.sharding import PartitionSpec as P

MESH = pl.DeviceIdType.MESH
F32, BF16 = jnp.float32, jnp.bfloat16

T, D, F, TOP = 256, 2048, 1408, 6
SLOTS, PAD, EXP = 30, 32, 4
ROWS = EXP * PAD
HALF = D // 2
PART = ((0, 88), (88, 88), (176, 80))
BIT = (4, 2, 1)
ORDER = tuple(tuple((p + i) % 3 for i in range(3)) for p in range(3))


def gather_messages(p):
    b0, b1, b2 = (BIT[d] for d in ORDER[p])
    table = ((0, 0), (0, 1), (b0, 1), (0, 2), (b0, 2), (b1, 2), (b0 | b1, 2))
    return tuple((s, i, s ^ BIT[ORDER[p][i]]) for s, i in table)


def scatter_messages(p):
    b0, b1, b2 = (BIT[d] for d in ORDER[p])
    return (
        (b0 | b1 | b2, 0, ()), (b0 | b1, 0, ()), (b0 | b2, 0, ()), (b0, 0, ()),
        (b1 | b2, 1, (0,)), (b1, 1, (1,)), (b2, 2, (2, 4)),
    )


GATHER = tuple(gather_messages(p) for p in range(3))
SCATTER = tuple(scatter_messages(p) for p in range(3))
GROUP = (None, 2, 2, 1, 2, 1, 1, 0)
LAST = (3, 5, 6)
PLACE = {0: 0, 1: 1, 2: 2, 4: 3}
WA, WB, WT = 768, 512, 128


def kernel(x, expert, slot, gate, wg, wu, wd, sg, su, sd, pt, rl, xg, *scratch):
    (ga, ua, gb, ub, gu, d0, d1, z, ds, ob, dr, r0, r1, r2, l0, l1, l2, s0, s1, s2, acc, xt, comb, h, mt, own, flat, ev, sv, gv,
     wsem, xsem, psem, tsem, xs_s, xs_r, meta_s, meta_r, ag_s, ag_r, fw_s, fw_r, dr_s, dr_r, own_s, own_r, rs_s, rs_r) = scratch
    me = lax.axis_index("ep")
    c, q = me % 2, me // 2
    sib = me + 1 - 2 * c
    nbr = [me + (1 - 2 * ((me // (2 * b)) % 2)) * (2 * b) for b in BIT]
    mine = pl.ds(pl.multiple_of(c * HALF, HALF), HALF)
    theirs = pl.ds(pl.multiple_of((1 - c) * HALF, HALF), HALF)
    rbuf, lbuf, sbuf = (r0, r1, r2), (l0, l1, l2), (s0, s1, s2)

    def remote(src, dst, send, recv, to):
        return pltpu.make_async_remote_copy(
            src_ref=src, dst_ref=dst, send_sem=send, recv_sem=recv, device_id={"ep": to}, device_id_type=MESH)

    def ag(k, p, m, first=False):
        s, i, land = GATHER[p][m]
        rows = pl.ds(*PART[p])
        src = x.at[rows, mine] if first else xg.at[k, s, rows, mine]
        return remote(src, xg.at[k, land, rows, mine], ag_s.at[k], ag_r.at[k, m], nbr[ORDER[p][i]])

    def ag_in(k, m):
        piece = xg.at[k, 0, :, mine]
        return remote(piece, piece, ag_s.at[k], ag_r.at[k, m], sib)

    def fwd(k, p, m):
        land = GATHER[p][m][2]
        piece = xg.at[k, land, pl.ds(*PART[p]), mine]
        return remote(piece, piece, fw_s.at[k], fw_r.at[k, land], sib)

    def fwd_in(k, r):
        piece = xg.at[k, r, :, theirs]
        return remote(piece, piece, fw_s.at[k], fw_r.at[k, r], sib)

    def gathered(k):
        sent = xg.at[k, pl.ds(0, 7), :, mine]
        return remote(sent, sent, ag_s.at[k], ag_r.at[k, 0], sib), remote(sent, sent, fw_s.at[k], fw_r.at[k, 0], sib)

    def give(k, r):
        return remote(ds.at[r], dr.at[k, r], dr_s.at[k], dr_r.at[k, GROUP[r]], sib)

    def give_in(k, n, g):
        return remote(ds.at[pl.ds(0, n)], dr.at[k, pl.ds(0, n)], dr_s.at[k], dr_r.at[k, g], sib)

    def give_own(half):
        return remote(ds.at[8 * half], dr.at[half, 0], own_s, own_r, sib)

    def gave_own():
        return remote(ds.at[pl.ds(0, 2)], dr.at[0, pl.ds(0, 2)], own_s, own_r, sib)

    def rs(k, p, n):
        to = nbr[ORDER[p][SCATTER[p][n][1]]]
        send = rs_s.at[k, n // 6]
        if n in LAST:
            land = rl.at[pl.ds(*PART[p]), mine] if n == LAST[2] else lbuf[p].at[LAST.index(n), c]
            return remote(sbuf[p].at[n], land, send, rs_r.at[c, n], to - c + k)
        return remote(sbuf[p].at[n], rbuf[p].at[k, PLACE[n]], send, rs_r.at[k, n], to)

    def rs_in(k, n):
        piece = rl.at[:, mine]
        return remote(piece, piece, rs_s.at[k, 0], rs_r.at[k, n], sib)

    def rs_sent(k, g):
        sent = xg.at[k, pl.ds(0, 1 if g else 6), :, mine]
        return remote(sent, sent, rs_s.at[k, g], rs_r.at[k, 0], sib)

    def meta_copy(i):
        return remote(own.at[i], mt.at[i], meta_s, meta_r, xor(me, i, 4))

    def meta_all():
        return remote(own.at[pl.ds(1, 15)], mt.at[pl.ds(1, 15)], meta_s, meta_r, sib)

    def xor(v, mask, bits):
        out = v
        for b in range(bits):
            if mask >> b & 1:
                out = out + (1 - 2 * ((v // (1 << b)) % 2)) * (1 << b)
        return out

    own_send = [remote(x.at[:, cols], xg.at[c, 0, :, cols], xs_s.at[n], xs_r.at[n], sib)
                for n, cols in enumerate((theirs, mine))]
    own_recv = [remote(x.at[:, cols], xg.at[1 - c, 0, :, cols], xs_s.at[n], xs_r.at[n], sib)
                for n, cols in enumerate((mine, theirs))]
    x_in = pltpu.make_async_copy(x, xt.at[0], xsem.at[0])

    def load_a(g, u):
        return [pltpu.make_async_copy(g(0, WA), ga, wsem.at[0]), pltpu.make_async_copy(u(0, WA), ua, wsem.at[1])]

    def load_b(g, u):
        return [
            pltpu.make_async_copy(g(WA, WB), gb, wsem.at[2]),
            pltpu.make_async_copy(u(WA, WB), ub, wsem.at[3]),
            pltpu.make_async_copy(g(WA + WB, WT), gu.at[:, pl.ds(0, WT)], wsem.at[4]),
            pltpu.make_async_copy(u(WA + WB, WT), gu.at[:, pl.ds(WT, WT)], wsem.at[5]),
        ]

    def load_d(d):
        return [pltpu.make_async_copy(d(n * HALF, HALF), (d0, d1)[n], wsem.at[6 + n]) for n in range(2)]

    def start(copies):
        for copy in copies:
            copy.start()

    def wait(copies):
        for copy in copies:
            copy.wait()

    def routed(ref, e):
        return lambda n, w: ref.at[e, :, pl.ds(n, w)]

    def shared_in(ref, i):
        return lambda n, w: ref.at[:, pl.ds(pl.multiple_of(i * F + n, 128), w)]

    def shared_out(i):
        return lambda n, w: sd.at[pl.ds(pl.multiple_of(i * F, 128), F), pl.ds(n, w)]

    def start_gather(k):
        @pl.when(c == k)
        def _():
            for m in (0, 1, 3):
                for p in range(3):
                    ag(k, p, m, first=True).start()

        @pl.when(c != k)
        def _():
            own_recv[0].wait_recv()
            for m in (0, 1, 3):
                for p in range(3):
                    ag(k, p, m).start()

    def arrive(k, m, sends):
        ag_in(k, m).wait_recv()
        for n in sends:
            for p in range(3):
                ag(k, p, n).start()
        for p in range(3):
            fwd(k, p, m).start()

    def x_load(k, r, b):
        return pltpu.make_async_copy(xg.at[k, r], xt.at[b], xsem.at[b])

    def fetch(k, r, b):
        if r:
            fwd_in(k, r).wait_recv()
            x_load(k, r, b).start()
            return

        @pl.when(c == k)
        def _():
            pltpu.make_async_copy(x, xt.at[b], xsem.at[b]).start()

        @pl.when(c != k)
        def _():
            own_recv[1].wait_recv()
            x_load(k, r, b).start()

    def dispatch(k, r, b):
        x_load(k, r, b).wait()
        table = mt[2 * r + (k + c) % 2].astype(F32)
        row = lax.broadcasted_iota(jnp.int32, (ROWS, T), 0).astype(F32)
        pick = jnp.zeros((ROWS, T), F32)
        weight = jnp.zeros((ROWS, T), F32)
        for j in range(TOP):
            hit = table[j:j + 1, :] == row
            pick = jnp.where(hit, 1.0, pick)
            weight = jnp.where(hit, table[8 + j:9 + j, :], weight)
        comb[k, r] = weight.T
        for n in range(0, D, 512):
            rows = jnp.dot(pick.astype(BF16), xt[b, :, n:n + 512], preferred_element_type=F32).astype(BF16)
            for e in range(EXP):
                z[e, r * PAD:(r + 1) * PAD, n:n + 512] = rows[e * PAD:(e + 1) * PAD]

    def gated(g, u):
        return (g * (1.0 / (1.0 + jnp.exp(-g))) * u).astype(BF16)

    def dot(a, b):
        return jnp.dot(a, b, preferred_element_type=F32)

    def hidden_a(load):
        for n in range(0, WA, 256):
            h[:, n:n + 256] = gated(dot(load(), ga[:, n:n + 256]), dot(load(), ua[:, n:n + 256]))

    def hidden_b(load):
        for n in range(0, WB, 256):
            h[:, WA + n:WA + n + 256] = gated(dot(load(), gb[:, n:n + 256]), dot(load(), ub[:, n:n + 256]))
        both = dot(load(), gu[...])
        h[:, WA + WB:] = gated(both[:, :WT], both[:, WT:])

    def down(store, halves=(0, 1)):
        for half in halves:
            for n in range(0, HALF, 512):
                store(half * HALF + n, dot(h[...], (d0, d1)[half][:, n:n + 512]))

    def give_some(k, rs):
        for r in rs:
            ds[r] = dot(comb[k, r].astype(BF16), ob[k, r, :, theirs]).astype(BF16)
            give(k, r).start()

    def give_owner(k):
        @pl.when(c != k)
        def _():
            for half in range(2):
                part = dot(comb[k, 0].astype(BF16), ob[k, 0, :, half * HALF:half * HALF + HALF])
                ds[8 * half] = part.astype(BF16)
                give_own(half).start()

    def gave_all(k):
        give_in(k, 7, 0).wait_send()

        @pl.when(c != k)
        def _():
            gave_own().wait_send()

    def term(k, p, r):
        first, rows = PART[p]
        low = first // 16 * 16
        part = dot(comb[k, r, first:first + rows, :].astype(BF16), ob[k, r, :, mine])
        other = dr[k, r, low:first + rows, :].astype(F32)[first - low:]
        return part + other

    def send_sum(k, n):
        for j in SCATTER[0][n][2]:
            rs_in(k, j).wait_recv()
        for p in range(3):
            r, _, joins = SCATTER[p][n]
            total = term(k, p, r)
            for j in joins:
                total = total + rbuf[p][k, PLACE[j]].astype(F32)
            sbuf[p][n] = total.astype(BF16)
            rs(k, p, n).start()

    def scatter(k, group, messages):
        give_in(k, 1 if group == 0 else 3, group).wait_recv()
        for n in messages:
            send_sum(k, n)

    def finish():
        gave_own().wait_recv()
        for half in range(2):
            cols = slice(half * HALF, half * HALF + HALF)
            acc[:, cols] += dot(comb[c, 0].astype(BF16), ob[c, 0, :, cols]) + dr[half, 0].astype(F32)

    def finish_arrived():
        for n in range(2):
            for half in range(2):
                rs_in(half, LAST[n]).wait_recv()
        for half in range(2):
            cols = slice(half * HALF, half * HALF + HALF)
            for p in range(3):
                first, rows = PART[p]
                acc[first:first + rows, cols] += lbuf[p][0, half].astype(F32) + lbuf[p][1, half].astype(F32)
        result.start()

    result = pltpu.make_async_copy(acc, pt, psem)

    tables = [pltpu.make_async_copy(a, b, tsem.at[n]) for n, (a, b) in enumerate(((expert, ev), (slot, sv), (gate, gv)))]
    start(tables)
    x_in.start()
    start(load_a(shared_in(sg, 0), shared_in(su, 0)))
    barrier = pltpu.get_barrier_semaphore()
    for i in range(1, 16):
        pl.semaphore_signal(barrier, inc=1, device_id={"ep": xor(me, i, 4)}, device_id_type=MESH)
    pl.semaphore_wait(barrier, 15)
    own_send[0].start()
    own_send[1].start()
    start_gather(0)
    start(load_b(shared_in(sg, 0), shared_in(su, 0)))
    start(load_d(shared_out(0)))

    wait(tables)
    flat[...] = jnp.full_like(flat, -1)
    for j in range(TOP):
        flat[j:j + 1, :] = jnp.where(sv[j] < SLOTS, ev[j] * PAD + sv[j], -1)
    gates = jnp.concatenate([gv[j] for j in range(TOP)] + [jnp.zeros((2, T), F32)], axis=0)
    for i in range(16):
        row = flat[...] - xor(me, i, 4) * ROWS
        row = jnp.where((row >= 0) & (row < ROWS), row, -1).astype(F32)
        own[i] = jnp.concatenate([row, gates], axis=0).astype(BF16)
    mt[0] = own[0]
    acc[...] = jnp.zeros_like(acc)
    for i in range(1, 16):
        meta_copy(i).start()
    x_in.wait()

    @pl.loop(0, 2)
    def _(i):
        def following(ref, routed_ref, load):
            @pl.when(i == 0)
            def _():
                start(load(*(shared_in(v, 1) for v in ref)))

            @pl.when(i == 1)
            def _():
                start(load(*(routed(v, 0) for v in routed_ref)))

        wait(load_a(shared_in(sg, i), shared_in(su, i)))
        hidden_a(lambda: xt[0])
        following((sg, su), (wg, wu), load_a)
        wait(load_b(shared_in(sg, i), shared_in(su, i)))
        hidden_b(lambda: xt[0])
        following((sg, su), (wg, wu), load_b)

        def store(n, v):
            acc[:, n:n + 512] += v

        wait(load_d(shared_out(i)))
        down(store)

        @pl.when(i == 0)
        def _():
            start(load_d(shared_out(1)))

        @pl.when(i == 1)
        def _():
            start(load_d(routed(wd, 0)))

        @pl.when(i == 0)
        def _():
            arrive(0, 0, (2, 4))

    arrive(0, 1, (5,))
    arrive(0, 3, ())
    meta_all().wait_recv()
    ORDER_IN = (0, 4, 2, 1, 6, 5, 3, 7)
    BUFFERS = 3

    def run(k, steps):
        for step in steps:
            if callable(step):
                step()
            elif step > 0:
                fetch(k, ORDER_IN[step - 1], (step - 1) % BUFFERS)
            else:
                dispatch(k, ORDER_IN[-step - 1], (-step - 1) % BUFFERS)

    run(0, (1, 2, lambda: arrive(0, 2, (6,)), lambda: start_gather(1), 3, -1, 4, -2, lambda: arrive(0, 4, ()), -3, -4,
            lambda: arrive(0, 5, ()), 5, 6, 7, -5, -6, -7, lambda: arrive(0, 6, ()), 8, -8))

    @pl.loop(0, 8)
    def _(i):
        k, e = i // 4, i % 4
        nxt = (i + 1) % 4
        wait(load_a(routed(wg, e), routed(wu, e)))
        hidden_a(lambda: z[e])
        @pl.when(i < 7)
        def _():
            start(load_a(routed(wg, nxt), routed(wu, nxt)))

        @pl.when(i == 7)
        def _():
            send_sum(0, 6)

        wait(load_b(routed(wg, e), routed(wu, e)))
        hidden_b(lambda: z[e])

        @pl.when(i < 7)
        def _():
            start(load_b(routed(wg, nxt), routed(wu, nxt)))

        @pl.when(i == 0)
        def _():
            arrive(1, 0, (2, 4))

        @pl.when(i == 3)
        def _():
            arrive(1, 4, ())
            run(1, (1, 2, 3))

        @pl.when(i == 4)
        def _():
            send_sum(0, 4)

        @pl.when(i == 5)
        def _():
            send_sum(0, 5)

        def store(n, v):
            for r in range(8):
                ob[k, r, pl.ds(pl.multiple_of(e * PAD, PAD), PAD), n:n + 512] = v[r * PAD:(r + 1) * PAD].astype(BF16)

        for half in range(2):
            wait(load_d(routed(wd, e))[half:half + 1])
            down(store, (half,))

            @pl.when(i < 7)
            def _():
                start(load_d(routed(wd, nxt))[half:half + 1])

        @pl.when(i == 1)
        def _():
            arrive(1, 1, (5,))

        @pl.when(i == 2)
        def _():
            arrive(1, 2, (6,))
            arrive(1, 3, ())

        @pl.when(i == 3)
        def _():
            run(1, (
                lambda: arrive(1, 5, ()), lambda: give_some(0, (7, 6, 5, 3)), lambda: arrive(1, 6, ()),
                -1, 4, -2, 5, lambda: scatter(0, 0, (0,)), lambda: give_some(0, (4, 2, 1)), lambda: give_owner(0),
                -3, 6, -4, 7, lambda: scatter(0, 1, (1, 2)), -5, 8, -6, -7,
                lambda: scatter(0, 2, (3,)), -8))


    gave_all(0)
    give_some(1, (7, 6, 5, 3, 4, 2, 1))
    rs_sent(0, 0).wait_send()
    scatter(1, 0, (0,))
    scatter(1, 1, (1, 2))
    scatter(1, 2, (3,))
    give_owner(1)
    send_sum(1, 4)
    send_sum(1, 5)
    finish()
    rs_sent(0, 1).wait_send()
    send_sum(1, 6)
    finish_arrived()

    result.wait()
    for copy in own_send:
        copy.wait_send()
    meta_all().wait_send()
    for k in range(2):
        for copies in gathered(k):
            copies.wait_send()
    gave_all(1)
    for g in range(2):
        rs_sent(1, g).wait_send()
    for half in range(2):
        rs_in(half, LAST[2]).wait_recv()


def solution(mesh):
    dma = pltpu.SemaphoreType.DMA

    def body(x, expert, slot, gate, wg, wu, wd, sg, su, sd):
        x = x.reshape(T, D)
        expert, slot, gate = (v.transpose(0, 3, 1, 2).reshape(TOP, 1, T) for v in (expert, slot, gate))
        hbm = pl.BlockSpec(memory_space=pltpu.HBM)
        own, others, _ = pl.pallas_call(
            kernel,
            name="moe",
            out_shape=(
                jax.ShapeDtypeStruct((T, D), F32), jax.ShapeDtypeStruct((T, D), BF16),
                jax.ShapeDtypeStruct((2, 8, T, D), BF16)),
            in_specs=[hbm, hbm, hbm, hbm, hbm, hbm, hbm, hbm, hbm, hbm],
            out_specs=(hbm, hbm, hbm),
            scratch_shapes=[
                *[pltpu.VMEM((D, n), BF16) for n in (WA, WA, WB, WB, 2 * WT)],
                *[pltpu.VMEM((F, HALF), BF16)] * 2,
                pltpu.VMEM((EXP, T, D), BF16),
                pltpu.VMEM((9, T, HALF), BF16),
                pltpu.VMEM((2, 8, ROWS, D), BF16),
                pltpu.VMEM((2, 8, T, HALF), BF16),
                *[pltpu.VMEM((2, 4, n, HALF), BF16) for _, n in PART],
                *[pltpu.VMEM((2, 2, n, HALF), BF16) for _, n in PART],
                *[pltpu.VMEM((7, n, HALF), BF16) for _, n in PART],
                pltpu.VMEM((T, D), F32),
                pltpu.VMEM((3, T, D), BF16),
                pltpu.VMEM((2, 8, T, ROWS), F32),
                pltpu.VMEM((T, F), BF16),
                pltpu.VMEM((16, 16, T), BF16), pltpu.VMEM((16, 16, T), BF16), pltpu.VMEM((8, T), jnp.int32),
                pltpu.VMEM((TOP, 1, T), jnp.int32), pltpu.VMEM((TOP, 1, T), jnp.int32), pltpu.VMEM((TOP, 1, T), F32),
                dma((8,)), dma((3,)), dma, dma((3,)), dma((2,)), dma((2,)), dma, dma,
                dma((2,)), dma((2, 7)), dma((2,)), dma((2, 8)), dma((2,)), dma((2, 3)), dma, dma,
                dma((2, 2)), dma((2, 7)),
            ],
            compiler_params=pltpu.CompilerParams(collective_id=0, has_side_effects=True, vmem_limit_bytes=67_043_328),
        )(x, expert, slot, gate, wg, wu, wd, sg, su, sd)
        return (own + others.astype(F32)).astype(BF16).reshape(1, 1, T, D)

    tokens, experts, whole = P("dp", "ep", None, None), P("ep", None, None), P(None, None)
    return jax.shard_map(
        body, mesh=mesh,
        in_specs=(tokens, tokens, tokens, tokens, experts, experts, experts, whole, whole, whole),
        out_specs=tokens, check_vma=False)
```
